32 devices in a mesh: dp: 8 (over z, y), mp: 4 (over x, core).
Axes of the slice: x: 2, y: 2, z: 4, core: 2. Of those that a mesh axis runs over, the one named last changes fastest.
Arguments:
- gradient: bfloat16 [8, 64, 14336], P('dp', None, 'mp'), may hold values from -6 to 6
- momentum: float32 [8, 64, 14336], P('dp', None, 'mp'), may hold values from -6 to 6
- weights: float32 [64, 14336], P(None, 'mp'), may hold values from -6 to 6
- positions: int32 [8, 1, 224, 32], P('dp', None, 'mp'), may hold values from 0 to 4095, as said below
Outputs:
- new_momentum: float32 [8, 64, 14336], P('dp', None, 'mp')
- new_weights: float32 [64, 14336], P(None, 'mp')
The draws below stay inside these ranges and needn't reach their ends.
Inputs may be any that keep to these rules, and one draw needn't show every extreme that they name: Within one span of one replica the 32 positions are all different.
All inputs are finite; a program needn't handle non-finite values.
Results may differ from the reference program's by a relative error of at most 0.0003.
Values sent between devices are 32-bit elements; how exact they have to be, the bound alone decides.
A program may use at most 64 MiB of HBM per device.

```python
import jax
import jax.numpy as jnp
from jax import lax

FF = 14336
BANDS = 1
K = 32
REPLICAS = 8
COLCH = 224


def draw_positions(key, part):
    scores = jax.random.randint(key, (REPLICAS, BANDS, FF // 64, 4096), 0, 262144, dtype=jnp.int32)
    scores = scores * 4096 + jnp.arange(4096, dtype=jnp.int32)
    chosen = jax.lax.top_k(scores, K)[1]
    return chosen.astype(jnp.int32)


def levels(own_key, dims, split, least, top_value):
    level, own = 1.0, jax.random.fold_in(own_key, 6)
    for dim, blocks in split:
        heights = jnp.exp(jax.random.uniform(jax.random.fold_in(own, dim), (blocks,), jnp.float32, least / len(split), top_value / len(split)))
        level = level * jnp.repeat(heights, dims[dim] // blocks).reshape([-1 if axis == dim else 1 for axis in range(len(dims))])
    return level


def normal_values(rng, extent, scale, most, shards=(), held_as=jnp.bfloat16):
    result = scale * jax.random.normal(rng, extent, jnp.float32)
    if shards:
        result = result * levels(rng, extent, shards, -0.22, 0.18)
    return jnp.clip(result, -most, most).astype(held_as)


def setup_inputs(seed: int = 0) -> dict:
    splits = jax.random.split(jax.random.key(seed), 5)
    gradient = normal_values(splits[0], (REPLICAS, 64 * BANDS, FF), 1.0, 6.0, ((0, 8), (2, 4)))
    momentum = normal_values(splits[1], (REPLICAS, 64 * BANDS, FF), 1.0, 6.0, ((0, 8), (2, 4)), jnp.float32)
    weights = normal_values(splits[2], (64 * BANDS, FF), 1.0, 6.0, ((1, 4),), jnp.float32)
    positions = draw_positions(jax.random.fold_in(splits[4], 71), 0)
    return {"gradient": gradient, "momentum": momentum, "weights": weights, "positions": positions}


def dct_table():
    column = jnp.arange(64, dtype=jnp.float32)
    freq = column[:, None]
    factor = jnp.where(freq == 0, jnp.sqrt(jnp.float32(1.0 / 64)), jnp.sqrt(jnp.float32(2.0 / 64)))
    return factor * jnp.cos(jnp.pi * (2.0 * column[None, :] + 1.0) * freq / 128.0)

def reference(gradient, momentum, weights, positions):
    table = dct_table()
    rows_all = 64 * BANDS
    band_index = jnp.arange(BANDS, dtype=jnp.int32)[:, None, None]
    span_index = jnp.arange(COLCH, dtype=jnp.int32)[None, :, None]

    def one_replica(carry, inputs):
        grad_one, mom_one, pos_one = inputs
        summed = 0.9 * mom_one + grad_one.astype(jnp.float32)
        blocks = summed.reshape(BANDS, 64, COLCH, 64)
        coefs = jnp.einsum('kr,brcs,ls->bckl', table, blocks, table, precision=lax.Precision.HIGHEST)
        flatten = coefs.reshape(BANDS, COLCH, 4096)
        picked = jnp.take_along_axis(flatten, pos_one, axis=2)
        own = jnp.zeros((BANDS, COLCH, 4096), jnp.float32).at[band_index, span_index, pos_one].add(picked)
        back = jnp.einsum('kr,bckl,ls->brcs', table, own.reshape(BANDS, COLCH, 64, 64), table, precision=lax.Precision.HIGHEST)
        return (carry + own, summed - back.reshape(rows_all, FF))
    start = jnp.zeros((BANDS, COLCH, 4096), jnp.float32)
    aggregate, new_momentum = lax.scan(one_replica, start, (gradient, momentum, positions))
    update = jnp.einsum('kr,bckl,ls->brcs', table, aggregate.reshape(BANDS, COLCH, 64, 64), table, precision=lax.Precision.HIGHEST)
    update = update.reshape(rows_all, FF)
    meansq = jnp.mean(update * update)
    new_weights = weights - update / jnp.sqrt(meansq + 1.0)
    return (new_momentum, new_weights)
```

```python
import functools

import jax
import jax.numpy as jnp
import numpy as np
from jax import lax
from jax.experimental import pallas as pl
from jax.experimental.pallas import tpu as pltpu
from jax.sharding import PartitionSpec as P

QUAD = 256
PAIR = 128
GROUP = 8
CHUNKS = 2
F32 = jnp.float32
BF16 = jnp.bfloat16


def dct_table():
    column = np.arange(64, dtype=np.float64)
    freq = column[:, None]
    factor = np.where(freq == 0, np.sqrt(1.0 / 64), np.sqrt(2.0 / 64))
    return factor * np.cos(np.pi * (2.0 * column[None, :] + 1.0) * freq / 128.0)


def halves(table):
    high = np.asarray(table, np.float32).astype(jnp.bfloat16)
    low = np.asarray(table - high.astype(np.float64), np.float32).astype(jnp.bfloat16)
    return high, low


def side_tables():
    table = dct_table()
    high, low = halves(table.T)
    gather = np.concatenate([high, low], axis=0)
    rows = np.concatenate([high, low, high, low], axis=1)
    columns = np.concatenate(halves(np.kron(np.eye(2), table)), axis=1)
    return gather, rows, columns


def split(value):
    high = value.astype(BF16)
    return high, (value - high.astype(F32)).astype(BF16)


def dot(a, b):
    return jnp.dot(a, b, preferred_element_type=F32)


def dot_t(a, b):
    return lax.dot_general(a, b, (((1,), (1,)), ((), ())), preferred_element_type=F32)


def row_transform(table, value):
    high, low = split(value)
    return dot(table, jnp.concatenate([high, high, low, low], axis=0))


def column_transform(both, table):
    result = dot(both, jnp.concatenate([table, table], axis=0))
    return result[:, :PAIR] + result[:, PAIR:]


def counting(rows, lanes):
    count = lax.broadcasted_iota(jnp.int32, (rows, lanes), 0).astype(F32)
    return count.astype(BF16).reshape(-1, 16, lanes)


def spread(row):
    return jnp.broadcast_to(row, (16, row.shape[1])).astype(BF16)[None]


def flat(tiles):
    return tiles.reshape(-1, tiles.shape[-1])


def frequencies(places):
    return (places // 64).astype(F32), (places % 64).astype(F32)


def lane_part(shape):
    return lax.broadcasted_iota(jnp.int32, shape, 1) // 32


def regroup(members, part):
    result = []
    for start in range(0, GROUP, 4):
        joined = None
        for place in range(4):
            member = members[start + place]
            shift = (place - part) % 4 * 32
            moved = pltpu.roll(member, shift, axis=1) if shift else member
            joined = moved if joined is None else jnp.where(lane_part(moved.shape) == place, moved, joined)
        result.append(joined)
    return jnp.concatenate(result, axis=1)


def loop(count, body):
    if count <= 16:
        for step in range(count):
            body(step)
    else:
        lax.fori_loop(0, count, lambda step, carry: (body(step), carry)[1], 0)


def kernel(
    replicas, parts, chunks,
    gradient_ref, momentum_ref, weights_ref, places_hbm, gather_hbm, rows_hbm, columns_hbm,
    summed, update, wts, squares,
    grad, mom, places_ref, gather_ref, rows_ref, columns_ref, flipped, row_side, column_side, both, coefs,
    place_lists, value_lists, row_parts, column_parts, value_parts,
    in_sem, chunk_sem, place_send, place_recv, value_send, value_recv, square_send, square_recv,
):
    me, mine = lax.axis_index("dp"), lax.axis_index("mp")
    width = summed.shape[1]
    quads = width // QUAD
    per = quads // chunks
    tall = place_lists.shape[1] // chunks

    def block(index):
        return pl.ds(index * QUAD, QUAD)

    def rows(index):
        return pl.ds(index * 64, 64)

    def line(index):
        return index // per * tall + index % per

    def chunk_loads(chunk):
        span = pl.ds(chunk * per * QUAD, per * QUAD)
        return [
            pltpu.make_async_copy(source.at[0, :, span], target.at[:, span], chunk_sem.at[chunk, index])
            for index, (source, target) in enumerate(((gradient_ref, grad), (momentum_ref, mom)))
        ]

    loads = [
        pltpu.make_async_copy(source, target, in_sem.at[index])
        for index, (source, target) in enumerate(
            (
                (places_hbm.at[0, 0], places_ref), (gather_hbm, gather_ref),
                (rows_hbm, rows_ref), (columns_hbm, columns_ref), (weights_ref, wts),
            )
        )
    ]
    for load in loads[:2]:
        load.start()
    for chunk in range(chunks):
        for load in chunk_loads(chunk):
            load.start()
    for load in loads[2:]:
        load.start()

    barrier = pltpu.get_barrier_semaphore()

    def greet_replica(step):
        pl.semaphore_signal(
            barrier, inc=1, device_id={"dp": lax.rem(me + step + 1, replicas)},
            device_id_type=pl.DeviceIdType.MESH,
        )

    def greet_part(step):
        pl.semaphore_signal(
            barrier, inc=1, device_id={"mp": lax.rem(mine + step + 1, parts)},
            device_id_type=pl.DeviceIdType.MESH,
        )

    loop(replicas - 1, greet_replica)
    loop(parts - 1, greet_part)

    def list_copy(lists, send_sem, recv_sem, step, slot, span):
        return pltpu.make_async_remote_copy(
            src_ref=lists.at[slot, span], dst_ref=lists.at[slot, span],
            send_sem=send_sem, recv_sem=recv_sem,
            device_id={"dp": lax.rem(me + step + 1, replicas)},
            device_id_type=pl.DeviceIdType.MESH,
        )

    def place_copy(step, slot):
        return list_copy(
            place_lists, place_send.at[step], place_recv.at[slot], step, slot, pl.ds(0, chunks * tall)
        )

    def value_copy(chunk, step, slot):
        return list_copy(
            value_lists, value_send.at[chunk, step], value_recv.at[chunk, slot],
            step, slot, pl.ds(chunk * tall, tall),
        )

    groups = place_lists.shape[0] // GROUP
    for slot in range(replicas, groups * GROUP):
        place_lists[slot, :, :] = jnp.zeros(place_lists.shape[1:], F32)
        value_lists[slot, :, :] = jnp.zeros(value_lists.shape[1:], F32)

    loads[0].wait()
    flipped[...] = jnp.transpose(places_ref[...])
    places = jnp.concatenate(
        [flipped[pl.ds(part, quads, stride=4), :] for part in range(4)], axis=1
    )
    for chunk in range(chunks):
        place_lists[me, chunk * tall : chunk * tall + per, :] = places[
            chunk * per : (chunk + 1) * per
        ].astype(F32)

    pl.semaphore_wait(barrier, replicas - 1 + parts - 1)
    loop(replicas - 1, lambda step: place_copy(step, me).start())

    zero, one = jnp.zeros((), BF16), jnp.ones((), BF16)
    count = counting(64, PAIR)
    row_freqs, column_freqs = frequencies(places)
    lanes = lane_part((64, PAIR))

    def hot(row):
        return flat(jnp.where(count == spread(row), one, zero))

    loads[1].wait()
    for index in range(quads):
        hots = [hot(freqs[index : index + 1, :]) for freqs in (row_freqs, column_freqs)]
        found = dot(gather_ref[...], jnp.concatenate(hots, axis=1))
        row_side[rows(index), :] = found[:64, :PAIR] + found[64:, :PAIR]
        for half in range(2):
            side = found[half * 64 : (half + 1) * 64, PAIR:]
            for part in range(4):
                column_side[pl.ds(index * QUAD + part * 64, 64), half * PAIR : (half + 1) * PAIR] = (
                    jnp.where(lanes == part, side, 0.0).astype(BF16)
                )

    for chunk in range(chunks):
        for load in chunk_loads(chunk):
            load.wait()
        for index in range(chunk * per, (chunk + 1) * per):
            value = 0.9 * mom[:, block(index)] + grad[:, block(index)].astype(F32)
            summed[:, block(index)] = value
            found = dot(jnp.concatenate(split(value), axis=0), column_side[block(index), :])
            found = found[:64, :] + found[64:, :]
            found = (found[:, :PAIR] + found[:, PAIR:]) * row_side[rows(index), :]
            value_lists[me, pl.ds(line(index), 1), :] = jnp.sum(found, axis=0, keepdims=True)
        loop(replicas - 1, lambda step: value_copy(chunk, step, me).start())

    for index in range(quads):
        scaled = row_side[rows(index), :] * value_lists[me, pl.ds(line(index), 1), :]
        high, low = split(scaled)
        left = jnp.concatenate(
            [jnp.concatenate([high, high], axis=1), jnp.concatenate([low, low], axis=1)], axis=0
        )
        back = dot_t(left, column_side[block(index), :])
        summed[:, block(index)] = summed[:, block(index)] - (back[:64, :] + back[64:, :])

    def source(step):
        return lax.rem(me + replicas - step - 1, replicas)

    def quad(ref, index):
        return jnp.concatenate([ref[rows(2 * index), :], ref[rows(2 * index + 1), :]], axis=1)

    def keep_pair(index, value):
        for half, part in enumerate(split(value)):
            both[rows(index), half * PAIR : (half + 1) * PAIR] = part

    def regroup_places(group):
        members = [
            frequencies(place_lists[group * GROUP + member, :, :].astype(jnp.int32))
            for member in range(GROUP)
        ]
        for part in range(4):
            row_parts[group, part, :, :] = regroup([member[0] for member in members], part)
            column_parts[group, part, :, :] = regroup([member[1] for member in members], part)

    def regroup_values(group, chunk):
        span = slice(chunk * tall, (chunk + 1) * tall)
        members = [value_lists[group * GROUP + member, span, :] for member in range(GROUP)]
        for part in range(4):
            value_parts[group, part, span, :] = regroup(members, part)

    loop(replicas - 1, lambda step: place_copy(step, source(step)).wait_recv())
    loop(groups, regroup_places)

    count_group = counting(64, GROUP * 32)

    def decode(group, index, part):
        place = slice(line(index), line(index) + 1)
        row_hot = flat(jnp.where(count_group == spread(row_parts[group, part, place, :]), one, zero))
        here = count_group == spread(column_parts[group, part, place, :])
        high, low = split(jnp.broadcast_to(value_parts[group, part, place, :], (16, GROUP * 32)))
        right = jnp.concatenate(
            [flat(jnp.where(here, high[None], zero)), flat(jnp.where(here, low[None], zero))], axis=0
        )
        result = dot_t(row_hot, right)
        return result + pltpu.roll(result, 64, axis=1)

    def decode_pair(group, index, side):
        left, right = (decode(group, index, 2 * side + place) for place in range(2))
        return jnp.where(lane_part(left.shape) < 2, left, right)

    square = jnp.zeros((8, PAIR), F32)
    for chunk in range(chunks):
        loop(replicas - 1, lambda step: value_copy(chunk, step, source(step)).wait_recv())
        loop(groups, lambda group: regroup_values(group, chunk))
        for index in range(chunk * per, (chunk + 1) * per):
            for side in range(2):
                total = decode_pair(0, index, side)
                if groups > 1:
                    total = lax.fori_loop(
                        1, groups, lambda step, acc: acc + decode_pair(step, index, side), total
                    )
                square = square + jnp.sum((total * total).reshape(8, 8, PAIR), axis=0)
                keep_pair(2 * index + side, total)

    squares[mine, :, :] = square

    def square_copy(step, slot):
        return pltpu.make_async_remote_copy(
            src_ref=squares.at[slot], dst_ref=squares.at[slot],
            send_sem=square_send.at[step], recv_sem=square_recv.at[slot],
            device_id={"mp": lax.rem(mine + step + 1, parts)},
            device_id_type=pl.DeviceIdType.MESH,
        )

    loop(parts - 1, lambda step: square_copy(step, mine).start())

    for load in loads[2:4]:
        load.wait()
    coefs[...] = column_transform(both[...], columns_ref[...])
    for index in range(quads):
        update[:, block(index)] = row_transform(rows_ref[...], quad(coefs, index))

    loads[4].wait()
    loop(replicas - 1, lambda step: place_copy(step, me).wait_send())
    for chunk in range(chunks):
        loop(replicas - 1, lambda step: value_copy(chunk, step, me).wait_send())
    loop(parts - 1, lambda step: square_copy(step, mine).wait_send())
    loop(
        parts - 1,
        lambda step: square_copy(step, lax.rem(mine + parts - step - 1, parts)).wait_recv(),
    )


def deliver(chunks, entries, summed, update, weights, squares, out_momentum_ref, out_weights_ref, result, out_sem):
    share = weights.shape[1] // chunks
    first = pltpu.make_async_copy(summed, out_momentum_ref.at[0], out_sem.at[chunks])
    first.start()
    meansq = jnp.sum(jnp.sum(squares[...], axis=0)) / entries
    factor = lax.rsqrt(jnp.full((1, share), meansq + 1.0, F32))
    stores = []
    for chunk in range(chunks):
        span = pl.ds(chunk * share, share)
        result[:, span] = weights[:, span] - update[:, span] * factor
        stores.append(pltpu.make_async_copy(result.at[:, span], out_weights_ref.at[:, span], out_sem.at[chunk]))
        stores[-1].start()
    first.wait()
    for store in stores:
        store.wait()


def local(replicas, parts, gradient, momentum, weights, positions):
    height, width = weights.shape
    quads = width // QUAD
    tables = side_tables()
    anywhere = pl.BlockSpec(memory_space=pl.ANY)
    vmem = pl.BlockSpec(memory_space=pltpu.VMEM)
    chunks = CHUNKS if quads % CHUNKS == 0 else 1
    listed = chunks * (-(-(quads // chunks) // 8) * 8)
    groups = -(-replicas // GROUP)
    entries = positions.shape[-1]
    wide = jax.ShapeDtypeStruct(weights.shape, F32)
    results = pl.pallas_call(
        functools.partial(kernel, replicas, parts, chunks),
        out_shape=(wide, wide, wide, jax.ShapeDtypeStruct((parts, 8, PAIR), F32)),
        in_specs=[pl.BlockSpec(memory_space=pltpu.HBM)] * 7,
        out_specs=(vmem,) * 4,
        scratch_shapes=[
            pltpu.VMEM((height, width), BF16),
            pltpu.VMEM((height, width), F32),
            pltpu.VMEM((entries, 4 * quads), jnp.int32),
            *[pltpu.VMEM(table.shape, BF16) for table in tables],
            pltpu.VMEM((4 * quads, entries), jnp.int32),
            pltpu.VMEM((quads * 64, PAIR), F32),
            pltpu.VMEM((quads * QUAD, QUAD), BF16),
            pltpu.VMEM((2 * quads * 64, QUAD), BF16),
            pltpu.VMEM((2 * quads * 64, PAIR), F32),
            pltpu.VMEM((groups * GROUP, listed, PAIR), F32),
            pltpu.VMEM((groups * GROUP, listed, PAIR), F32),
            pltpu.VMEM((groups, 4, listed, GROUP * 32), F32),
            pltpu.VMEM((groups, 4, listed, GROUP * 32), F32),
            pltpu.VMEM((groups, 4, listed, GROUP * 32), F32),
            pltpu.SemaphoreType.DMA((5,)),
            pltpu.SemaphoreType.DMA((chunks, 2)),
            pltpu.SemaphoreType.DMA((replicas,)),
            pltpu.SemaphoreType.DMA((replicas,)),
            pltpu.SemaphoreType.DMA((chunks, replicas)),
            pltpu.SemaphoreType.DMA((chunks, replicas)),
            pltpu.SemaphoreType.DMA((parts,)),
            pltpu.SemaphoreType.DMA((parts,)),
        ],
        compiler_params=pltpu.CompilerParams(
            collective_id=0, has_side_effects=True, vmem_limit_bytes=24 * 1024 * 1024
        ),
    )(
        *(
            pltpu.with_memory_space_constraint(array, pltpu.HBM)
            for array in (
                gradient, momentum, weights, jnp.swapaxes(positions, 2, 3), *map(jnp.asarray, tables),
            )
        )
    )
    return pl.pallas_call(
        functools.partial(deliver, chunks, float(height * width * parts)),
        out_shape=(
            jax.ShapeDtypeStruct(momentum.shape, F32),
            jax.ShapeDtypeStruct(weights.shape, F32),
        ),
        in_specs=[vmem] * 4,
        out_specs=(anywhere, anywhere),
        scratch_shapes=[pltpu.VMEM((height, width), F32), pltpu.SemaphoreType.DMA((chunks + 1,))],
        compiler_params=pltpu.CompilerParams(vmem_limit_bytes=8 * 1024 * 1024),
    )(*results)


def solution(mesh):
    placed = (P("dp", None, "mp"), P("dp", None, "mp"), P(None, "mp"), P("dp", None, "mp", None))
    return jax.shard_map(
        functools.partial(local, mesh.shape["dp"], mesh.shape["mp"]),
        mesh=mesh,
        in_specs=placed,
        out_specs=(P("dp", None, "mp"), P(None, "mp")),
        check_vma=False,
    )
```

```python
import functools

import jax
import jax.numpy as jnp
import numpy as np
from jax import lax
from jax.experimental import pallas as pl
from jax.experimental.pallas import tpu as pltpu
from jax.sharding import PartitionSpec as P

QUAD = 256
PAIR = 128
GROUP = 8
CHUNKS = 1
F32 = jnp.float32
BF16 = jnp.bfloat16
F8 = jnp.float8_e4m3fn


def dct_table():
    column = np.arange(64, dtype=np.float64)
    freq = column[:, None]
    factor = np.where(freq == 0, np.sqrt(1.0 / 64), np.sqrt(2.0 / 64))
    return factor * np.cos(np.pi * (2.0 * column[None, :] + 1.0) * freq / 128.0)


def halves(table):
    high = np.asarray(table, np.float32).astype(jnp.bfloat16)
    low = np.asarray(table - high.astype(np.float64), np.float32).astype(jnp.bfloat16)
    return high, low


def side_tables():
    table = dct_table()
    high, low = halves(table.T)
    gather = np.concatenate([high, low], axis=0)
    rows = np.concatenate([high, low, high, low], axis=1)
    columns = np.concatenate(halves(np.kron(np.eye(2), table)), axis=1)
    return gather, rows, columns


def split(value):
    high = value.astype(BF16)
    return high, (value - high.astype(F32)).astype(BF16)


def dot(a, b):
    return jnp.dot(a, b, preferred_element_type=F32)


def dot_t(a, b):
    return lax.dot_general(a, b, (((1,), (1,)), ((), ())), preferred_element_type=F32)


def row_transform(table, value):
    high, low = split(value)
    return dot(table, jnp.concatenate([high, high, low, low], axis=0))


def column_transform(both, table):
    result = dot(both, jnp.concatenate([table, table], axis=0))
    return result[:, :PAIR] + result[:, PAIR:]


def counting(rows, lanes):
    count = lax.broadcasted_iota(jnp.int32, (rows, lanes), 0).astype(F32)
    return count.astype(BF16).reshape(-1, 16, lanes)


def spread(row):
    return jnp.broadcast_to(row, (16, row.shape[1])).astype(BF16)[None]


def flat(tiles):
    return tiles.reshape(-1, tiles.shape[-1])


def frequencies(places):
    return (places // 64).astype(F32), (places % 64).astype(F32)


def lane_part(shape):
    return lax.broadcasted_iota(jnp.int32, shape, 1) // 32


def regroup(members, part):
    result = []
    for start in range(0, GROUP, 4):
        joined = None
        for place in range(4):
            member = members[start + place]
            shift = (place - part) % 4 * 32
            moved = pltpu.roll(member, shift, axis=1) if shift else member
            joined = moved if joined is None else jnp.where(lane_part(moved.shape) == place, moved, joined)
        result.append(joined)
    return jnp.concatenate(result, axis=1)


def loop(count, body):
    if count <= 16:
        for step in range(count):
            body(step)
    else:
        lax.fori_loop(0, count, lambda step, carry: (body(step), carry)[1], 0)


def each(count, body):
    if count == 1:
        body(0)
    else:
        lax.fori_loop(0, count, lambda step, carry: (body(step), carry)[1], 0)


def kernel(
    replicas, parts, chunks,
    gradient_ref, momentum_ref, weights_ref, places_hbm, gather_hbm, rows_hbm, columns_hbm,
    summed, update, wts, squares,
    grad, mom, places_ref, gather_ref, rows_ref, columns_ref, flipped, row_side, column_side, both, coefs,
    place_lists, value_lists, low_parts, cell_parts, value_parts, hots, sums,
    in_sem, chunk_sem, place_send, place_recv, value_send, value_recv, square_send, square_recv,
):
    me, mine = lax.axis_index("dp"), lax.axis_index("mp")
    width = summed.shape[1]
    quads = width // QUAD
    per = quads // chunks
    tall = place_lists.shape[1] // chunks

    def block(index):
        return pl.ds(index * QUAD, QUAD)

    def rows(index):
        return pl.ds(index * 64, 64)

    def line(index):
        return index // per * tall + index % per

    def chunk_loads(chunk):
        span = pl.ds(chunk * per * QUAD, per * QUAD)
        return [
            pltpu.make_async_copy(source.at[0, :, span], target.at[:, span], chunk_sem.at[chunk, index])
            for index, (source, target) in enumerate(((gradient_ref, grad), (momentum_ref, mom)))
        ]

    loads = [
        pltpu.make_async_copy(source, target, in_sem.at[index])
        for index, (source, target) in enumerate(
            (
                (places_hbm.at[0, 0], places_ref), (gather_hbm, gather_ref),
                (rows_hbm, rows_ref), (columns_hbm, columns_ref), (weights_ref, wts),
            )
        )
    ]
    for load in loads[:2]:
        load.start()
    for chunk in range(chunks):
        for load in chunk_loads(chunk):
            load.start()
    for load in loads[2:]:
        load.start()

    barrier = pltpu.get_barrier_semaphore()

    def greet_replica(step):
        pl.semaphore_signal(
            barrier, inc=1, device_id={"dp": lax.rem(me + step + 1, replicas)},
            device_id_type=pl.DeviceIdType.MESH,
        )

    def greet_part(step):
        pl.semaphore_signal(
            barrier, inc=1, device_id={"mp": lax.rem(mine + step + 1, parts)},
            device_id_type=pl.DeviceIdType.MESH,
        )

    loop(replicas - 1, greet_replica)
    loop(parts - 1, greet_part)

    def list_copy(lists, send_sem, recv_sem, step, slot, span):
        return pltpu.make_async_remote_copy(
            src_ref=lists.at[slot, span], dst_ref=lists.at[slot, span],
            send_sem=send_sem, recv_sem=recv_sem,
            device_id={"dp": lax.rem(me + step + 1, replicas)},
            device_id_type=pl.DeviceIdType.MESH,
        )

    def place_copy(step, slot):
        return list_copy(
            place_lists, place_send.at[step], place_recv.at[slot], step, slot, pl.ds(0, chunks * tall)
        )

    def value_copy(chunk, step, slot):
        return list_copy(
            value_lists, value_send.at[chunk, step], value_recv.at[chunk, slot],
            step, slot, pl.ds(chunk * tall, tall),
        )

    groups = place_lists.shape[0] // GROUP
    for slot in range(replicas, groups * GROUP):
        place_lists[slot, :, :] = jnp.zeros(place_lists.shape[1:], F32)
        value_lists[slot, :, :] = jnp.zeros(value_lists.shape[1:], F32)

    loads[0].wait()
    flipped[...] = jnp.transpose(places_ref[...])
    places = jnp.concatenate(
        [flipped[pl.ds(part, quads, stride=4), :] for part in range(4)], axis=1
    )
    for chunk in range(chunks):
        place_lists[me, chunk * tall : chunk * tall + per, :] = places[
            chunk * per : (chunk + 1) * per
        ].astype(F32)

    zero, one = jnp.zeros((), BF16), jnp.ones((), BF16)
    count = counting(64, PAIR)
    row_freqs, column_freqs = frequencies(places)
    lanes = lane_part((64, PAIR))

    def hot(row):
        return flat(jnp.where(count == spread(row), one, zero))

    loads[1].wait()
    for index in range(quads):
        pair = [hot(freqs[index : index + 1, :]) for freqs in (row_freqs, column_freqs)]
        found = dot(gather_ref[...], jnp.concatenate(pair, axis=1))
        row_side[rows(index), :] = found[:64, :PAIR] + found[64:, :PAIR]
        for half in range(2):
            side = found[half * 64 : (half + 1) * 64, PAIR:]
            for part in range(4):
                column_side[pl.ds(index * QUAD + part * 64, 64), half * PAIR : (half + 1) * PAIR] = (
                    jnp.where(lanes == part, side, 0.0).astype(BF16)
                )

    pl.semaphore_wait(barrier, replicas - 1 + parts - 1)
    loop(replicas - 1, lambda step: place_copy(step, me).start())

    for chunk in range(chunks):
        for load in chunk_loads(chunk):
            load.wait()
        for index in range(chunk * per, (chunk + 1) * per):
            value = 0.9 * mom[:, block(index)] + grad[:, block(index)].astype(F32)
            summed[:, block(index)] = value
            found = dot(jnp.concatenate(split(value), axis=0), column_side[block(index), :])
            found = found[:64, :] + found[64:, :]
            found = (found[:, :PAIR] + found[:, PAIR:]) * row_side[rows(index), :]
            value_lists[me, pl.ds(line(index), 1), :] = jnp.sum(found, axis=0, keepdims=True)
        loop(replicas - 1, lambda step: value_copy(chunk, step, me).start())

    def source(step):
        return lax.rem(me + replicas - step - 1, replicas)

    def quad(ref, index):
        return jnp.concatenate([ref[rows(2 * index), :], ref[rows(2 * index + 1), :]], axis=1)

    def keep_pair(index, value):
        for half, part in enumerate(split(value)):
            both[rows(index), half * PAIR : (half + 1) * PAIR] = part

    def regroup_places(group):
        low, cell = [], []
        for member in range(GROUP):
            spots = place_lists[group * GROUP + member, :, :].astype(jnp.int32)
            low.append((spots // 64 % 32).astype(F32))
            cell.append((spots // 2048 * 64 + spots % 64).astype(F32))
        for part in range(4):
            low_parts[group, part, :, :] = regroup(low, part)
            cell_parts[group, part, :, :] = regroup(cell, part)

    def regroup_values(group, chunk):
        span = slice(chunk * tall, (chunk + 1) * tall)
        members = [value_lists[group * GROUP + member, span, :] for member in range(GROUP)]
        for part in range(4):
            value_parts[group, part, span, :] = regroup(members, part)

    loop(replicas - 1, lambda step: place_copy(step, source(step)).wait_recv())
    spans = 4 * quads
    count_cell, count_low = counting(PAIR, GROUP * 32), counting(32, GROUP * 32)

    def cells(group, span):
        return pl.ds(pl.multiple_of((group * spans + span) * PAIR, PAIR), PAIR)

    def mark(group):
        regroup_places(group)
        for span in range(spans):
            cell = cell_parts[group, span % 4, pl.ds(line(span // 4), 1), :]
            hots[cells(group, span), :] = flat(
                jnp.where(count_cell == spread(cell), one, zero)
            ).astype(F8)

    def decode(group, span):
        place = pl.ds(line(span // 4), 1)
        here = count_low == spread(low_parts[group, span % 4, place, :])
        halves = split(jnp.broadcast_to(value_parts[group, span % 4, place, :], (16, GROUP * 32)))
        left = jnp.concatenate([flat(jnp.where(here, half[None], zero)) for half in halves], axis=0)
        result = dot_t(left, hots[cells(group, span), :])
        return result[:32, :] + result[32:, :]

    each(groups, mark)

    square = jnp.zeros((8, PAIR), F32)
    for chunk in range(chunks):
        loop(replicas - 1, lambda step: value_copy(chunk, step, source(step)).wait_recv())
        each(groups, lambda group: regroup_values(group, chunk))
        for span in range(chunk * per * 4, (chunk + 1) * per * 4):
            total = decode(0, span)
            if groups > 1:
                total = lax.fori_loop(1, groups, lambda step, acc: acc + decode(step, span), total)
            square = square + jnp.sum((total * total).reshape(4, 8, PAIR), axis=0)
            sums[pl.ds(span * 32, 32), :] = total

    squares[mine, :, :] = square

    def square_copy(step, slot):
        return pltpu.make_async_remote_copy(
            src_ref=squares.at[slot], dst_ref=squares.at[slot],
            send_sem=square_send.at[step], recv_sem=square_recv.at[slot],
            device_id={"mp": lax.rem(mine + step + 1, parts)},
            device_id_type=pl.DeviceIdType.MESH,
        )

    loop(parts - 1, lambda step: square_copy(step, mine).start())

    for load in loads[2:4]:
        load.wait()
    first = lane_part((32, PAIR)) < 2
    for pair in range(2 * quads):
        left, right = (sums[pl.ds((2 * pair + side) * 32, 32), :] for side in range(2))
        top = jnp.where(first, left, pltpu.roll(right, 64, axis=1))
        bottom = jnp.where(first, pltpu.roll(left, 64, axis=1), right)
        keep_pair(pair, jnp.concatenate([top, bottom], axis=0))
    coefs[...] = column_transform(both[...], columns_ref[...])
    for index in range(quads):
        update[:, block(index)] = row_transform(rows_ref[...], quad(coefs, index))
    for index in range(quads):
        scaled = row_side[rows(index), :] * value_lists[me, pl.ds(line(index), 1), :]
        high, low = split(scaled)
        left = jnp.concatenate(
            [jnp.concatenate([high, high], axis=1), jnp.concatenate([low, low], axis=1)], axis=0
        )
        back = dot_t(left, column_side[block(index), :])
        summed[:, block(index)] = summed[:, block(index)] - (back[:64, :] + back[64:, :])

    loads[4].wait()
    loop(replicas - 1, lambda step: place_copy(step, me).wait_send())
    for chunk in range(chunks):
        loop(replicas - 1, lambda step: value_copy(chunk, step, me).wait_send())
    loop(parts - 1, lambda step: square_copy(step, mine).wait_send())
    loop(
        parts - 1,
        lambda step: square_copy(step, lax.rem(mine + parts - step - 1, parts)).wait_recv(),
    )


def deliver(chunks, entries, summed, update, weights, squares, out_momentum_ref, out_weights_ref, result, out_sem):
    share = weights.shape[1] // chunks
    first = pltpu.make_async_copy(summed, out_momentum_ref.at[0], out_sem.at[chunks])
    first.start()
    meansq = jnp.sum(jnp.sum(squares[...], axis=0)) / entries
    factor = lax.rsqrt(jnp.full((1, share), meansq + 1.0, F32))
    stores = []
    for chunk in range(chunks):
        span = pl.ds(chunk * share, share)
        result[:, span] = weights[:, span] - update[:, span] * factor
        stores.append(pltpu.make_async_copy(result.at[:, span], out_weights_ref.at[:, span], out_sem.at[chunk]))
        stores[-1].start()
    first.wait()
    for store in stores:
        store.wait()


def local(replicas, parts, gradient, momentum, weights, positions):
    height, width = weights.shape
    quads = width // QUAD
    tables = side_tables()
    anywhere = pl.BlockSpec(memory_space=pl.ANY)
    vmem = pl.BlockSpec(memory_space=pltpu.VMEM)
    chunks = CHUNKS if quads % CHUNKS == 0 else 1
    listed = chunks * (-(-(quads // chunks) // 8) * 8)
    groups = -(-replicas // GROUP)
    entries = positions.shape[-1]
    wide = jax.ShapeDtypeStruct(weights.shape, F32)
    results = pl.pallas_call(
        functools.partial(kernel, replicas, parts, chunks),
        out_shape=(wide, wide, wide, jax.ShapeDtypeStruct((parts, 8, PAIR), F32)),
        in_specs=[pl.BlockSpec(memory_space=pltpu.HBM)] * 7,
        out_specs=(vmem,) * 4,
        scratch_shapes=[
            pltpu.VMEM((height, width), BF16),
            pltpu.VMEM((height, width), F32),
            pltpu.VMEM((entries, 4 * quads), jnp.int32),
            *[pltpu.VMEM(table.shape, BF16) for table in tables],
            pltpu.VMEM((4 * quads, entries), jnp.int32),
            pltpu.VMEM((quads * 64, PAIR), F32),
            pltpu.VMEM((quads * QUAD, QUAD), BF16),
            pltpu.VMEM((2 * quads * 64, QUAD), BF16),
            pltpu.VMEM((2 * quads * 64, PAIR), F32),
            pltpu.VMEM((groups * GROUP, listed, PAIR), F32),
            pltpu.VMEM((groups * GROUP, listed, PAIR), F32),
            pltpu.VMEM((groups, 4, listed, GROUP * 32), F32),
            pltpu.VMEM((groups, 4, listed, GROUP * 32), F32),
            pltpu.VMEM((groups, 4, listed, GROUP * 32), F32),
            pltpu.VMEM((groups * 4 * quads * PAIR, GROUP * 32), F8),
            pltpu.VMEM((4 * quads * 32, PAIR), F32),
            pltpu.SemaphoreType.DMA((5,)),
            pltpu.SemaphoreType.DMA((chunks, 2)),
            pltpu.SemaphoreType.DMA((replicas,)),
            pltpu.SemaphoreType.DMA((replicas,)),
            pltpu.SemaphoreType.DMA((chunks, replicas)),
            pltpu.SemaphoreType.DMA((chunks, replicas)),
            pltpu.SemaphoreType.DMA((parts,)),
            pltpu.SemaphoreType.DMA((parts,)),
        ],
        compiler_params=pltpu.CompilerParams(
            collective_id=0, has_side_effects=True, vmem_limit_bytes=(22 + 2 * groups) * 1024 * 1024
        ),
    )(
        *(
            pltpu.with_memory_space_constraint(array, pltpu.HBM)
            for array in (
                gradient, momentum, weights, jnp.swapaxes(positions, 2, 3), *map(jnp.asarray, tables),
            )
        )
    )
    return pl.pallas_call(
        functools.partial(deliver, chunks, float(height * width * parts)),
        out_shape=(
            jax.ShapeDtypeStruct(momentum.shape, F32),
            jax.ShapeDtypeStruct(weights.shape, F32),
        ),
        in_specs=[vmem] * 4,
        out_specs=(anywhere, anywhere),
        scratch_shapes=[pltpu.VMEM((height, width), F32), pltpu.SemaphoreType.DMA((chunks + 1,))],
        compiler_params=pltpu.CompilerParams(vmem_limit_bytes=8 * 1024 * 1024),
    )(*results)


def solution(mesh):
    placed = (P("dp", None, "mp"), P("dp", None, "mp"), P(None, "mp"), P("dp", None, "mp", None))
    return jax.shard_map(
        functools.partial(local, mesh.shape["dp"], mesh.shape["mp"]),
        mesh=mesh,
        in_specs=placed,
        out_specs=(P("dp", None, "mp"), P(None, "mp")),
        check_vma=False,
    )
```

```python
import functools

import jax
import jax.numpy as jnp
import numpy as np
from jax import lax
from jax.experimental import pallas as pl
from jax.experimental.pallas import tpu as pltpu
from jax.sharding import PartitionSpec as P

QUAD = 256
PAIR = 128
GROUP = 8
CHUNKS = 1
F32 = jnp.float32
BF16 = jnp.bfloat16
F8 = jnp.float8_e4m3fn


def dct_table():
    column = np.arange(64, dtype=np.float64)
    freq = column[:, None]
    factor = np.where(freq == 0, np.sqrt(1.0 / 64), np.sqrt(2.0 / 64))
    return factor * np.cos(np.pi * (2.0 * column[None, :] + 1.0) * freq / 128.0)


def halves(table):
    high = np.asarray(table, np.float32).astype(jnp.bfloat16)
    low = np.asarray(table - high.astype(np.float64), np.float32).astype(jnp.bfloat16)
    return high, low


def side_tables():
    table = dct_table()
    high, low = halves(table.T)
    gather = np.concatenate([high, low], axis=1)
    rows = np.concatenate([high, low, high, low], axis=1)
    columns = np.concatenate(halves(np.kron(np.eye(2), table)), axis=1)
    return gather, rows, columns


def split(value):
    high = value.astype(BF16)
    return high, (value - high.astype(F32)).astype(BF16)


def dot(a, b):
    return jnp.dot(a, b, preferred_element_type=F32)


def dot_t(a, b):
    return lax.dot_general(a, b, (((1,), (1,)), ((), ())), preferred_element_type=F32)


def row_transform(table, value):
    high, low = split(value)
    return dot(table, jnp.concatenate([high, high, low, low], axis=0))


def column_transform(both, table):
    result = dot(both, jnp.concatenate([table, table], axis=0))
    return result[:, :PAIR] + result[:, PAIR:]


def counting(rows, lanes):
    count = lax.broadcasted_iota(jnp.int32, (rows, lanes), 0).astype(F32)
    return count.astype(BF16).reshape(-1, 16, lanes)


def spread(row):
    return jnp.broadcast_to(row, (16, row.shape[1])).astype(BF16)[None]


def flat(tiles):
    return tiles.reshape(-1, tiles.shape[-1])


def frequencies(places):
    return (places // 64).astype(F32), (places % 64).astype(F32)


def lane_part(shape):
    return lax.broadcasted_iota(jnp.int32, shape, 1) // 32


def regroup(members, part):
    result = []
    for start in range(0, GROUP, 4):
        joined = members[start + -part % 4]
        for place in range(1, 4):
            member = members[start + (place - part) % 4]
            joined = jnp.where(lane_part(joined.shape) == place, member, joined)
        result.append(joined)
    return jnp.concatenate(result, axis=1)


def partners(me, count):
    if count > 16 or count & (count - 1):
        return (
            lambda step: lax.rem(me + step + 1, count),
            lambda step: lax.rem(me + count - step - 1, count),
        )
    bits = [1 << bit for bit in range(count.bit_length() - 1)]
    flips = {bit: bit * (1 - 2 * lax.rem(me // bit, 2)) for bit in bits}

    def across(step):
        return me + sum(flips[bit] for bit in bits if (count - 1 - step) & bit)

    return across, across


def loop(count, body):
    if count <= 16:
        for step in range(count):
            body(step)
    else:
        lax.fori_loop(0, count, lambda step, carry: (body(step), carry)[1], 0)


def each(count, body):
    if count == 1:
        body(0)
    else:
        lax.fori_loop(0, count, lambda step, carry: (body(step), carry)[1], 0)


def kernel(
    replicas, parts, chunks,
    gradient_ref, momentum_ref, weights_ref, places_hbm, gather_hbm, rows_hbm, columns_hbm,
    summed, update, wts, squares,
    grad, mom, places_ref, gather_ref, rows_ref, columns_ref, flipped, row_side, column_side, both, coefs,
    place_lists, value_lists, low_parts, cell_parts, value_parts, hots, sums,
    in_sem, chunk_sem, place_send, place_recv, value_send, value_recv, square_send, square_recv,
):
    me, mine = lax.axis_index("dp"), lax.axis_index("mp")
    width = summed.shape[1]
    quads = width // QUAD
    per = quads // chunks
    tall = place_lists.shape[1] // chunks

    def block(index):
        return pl.ds(index * QUAD, QUAD)

    def rows(index):
        return pl.ds(index * 64, 64)

    def line(index):
        return index // per * tall + index % per

    def chunk_loads(chunk):
        span = pl.ds(chunk * per * QUAD, per * QUAD)
        return [
            pltpu.make_async_copy(source.at[0, :, span], target.at[:, span], chunk_sem.at[chunk, index])
            for index, (source, target) in enumerate(((gradient_ref, grad), (momentum_ref, mom)))
        ]

    loads = [
        pltpu.make_async_copy(source, target, in_sem.at[index])
        for index, (source, target) in enumerate(
            (
                (places_hbm.at[0, 0], places_ref), (gather_hbm, gather_ref),
                (rows_hbm, rows_ref), (columns_hbm, columns_ref), (weights_ref, wts),
            )
        )
    ]
    for load in loads[:2]:
        load.start()
    for chunk in range(chunks):
        for load in chunk_loads(chunk):
            load.start()
    for load in loads[2:]:
        load.start()

    barrier = pltpu.get_barrier_semaphore()
    replica, source = partners(me, replicas)
    other_part, part_source = partners(mine, parts)

    def greet_replica(step):
        pl.semaphore_signal(
            barrier, inc=1, device_id={"dp": replica(step)},
            device_id_type=pl.DeviceIdType.MESH,
        )

    def greet_part(step):
        pl.semaphore_signal(
            barrier, inc=1, device_id={"mp": other_part(step)},
            device_id_type=pl.DeviceIdType.MESH,
        )

    loop(replicas - 1, greet_replica)
    loop(parts - 1, greet_part)

    def list_copy(lists, send_sem, recv_sem, step, slot, span):
        return pltpu.make_async_remote_copy(
            src_ref=lists.at[slot, span], dst_ref=lists.at[slot, span],
            send_sem=send_sem, recv_sem=recv_sem,
            device_id={"dp": replica(step)},
            device_id_type=pl.DeviceIdType.MESH,
        )

    def place_copy(step, slot):
        return list_copy(
            place_lists, place_send.at[step], place_recv.at[slot], step, slot, pl.ds(0, chunks * tall)
        )

    def value_copy(chunk, step, slot):
        return list_copy(
            value_lists, value_send.at[chunk, step], value_recv.at[chunk, slot],
            step, slot, pl.ds(chunk * tall, tall),
        )

    groups = place_lists.shape[0] // GROUP
    for slot in range(replicas, groups * GROUP):
        place_lists[slot, :, :] = jnp.zeros(place_lists.shape[1:], F32)
        value_lists[slot, :, :] = jnp.zeros(value_lists.shape[1:], F32)

    loads[0].wait()
    flipped[...] = jnp.transpose(places_ref[...])
    turn = lax.rem(me, 4)
    places = jnp.concatenate(
        [flipped[pl.ds(lax.rem(place + 4 - turn, 4), quads, stride=4), :] for place in range(4)], axis=1
    )
    for chunk in range(chunks):
        place_lists[me, chunk * tall : chunk * tall + per, :] = places[
            chunk * per : (chunk + 1) * per
        ].astype(F32)

    zero, one = jnp.zeros((), BF16), jnp.ones((), BF16)
    count = counting(64, PAIR)
    row_freqs, column_freqs = frequencies(places)
    lanes = lax.rem(lane_part((64, PAIR)) + 4 - turn, 4)

    def hot(row):
        return flat(jnp.where(count == spread(row), one, zero))

    loads[1].wait()
    for index in range(quads):
        pair = [hot(freqs[index : index + 1, :]) for freqs in (row_freqs, column_freqs)]
        both_hot = jnp.concatenate(pair, axis=1)
        found = dot(gather_ref[...], jnp.concatenate([both_hot, both_hot], axis=0))
        row_side[rows(index), :] = found[:, :PAIR]
        for half, side in enumerate(split(found[:, PAIR:])):
            for part in range(4):
                column_side[pl.ds(index * QUAD + part * 64, 64), half * PAIR : (half + 1) * PAIR] = (
                    jnp.where(lanes == part, side, zero)
                )

    pl.semaphore_wait(barrier, replicas - 1 + parts - 1)
    loop(replicas - 1, lambda step: place_copy(step, me).start())

    for chunk in range(chunks):
        for load in chunk_loads(chunk):
            load.wait()
        for index in range(chunk * per, (chunk + 1) * per):
            value = 0.9 * mom[:, block(index)] + grad[:, block(index)].astype(F32)
            summed[:, block(index)] = value
            found = dot(jnp.concatenate(split(value), axis=0), column_side[block(index), :])
            found = found[:64, :] + found[64:, :]
            found = (found[:, :PAIR] + found[:, PAIR:]) * row_side[rows(index), :]
            value_lists[me, pl.ds(line(index), 1), :] = jnp.sum(found, axis=0, keepdims=True)
        loop(replicas - 1, lambda step: value_copy(chunk, step, me).start())

    def quad(ref, index):
        return jnp.concatenate([ref[rows(2 * index), :], ref[rows(2 * index + 1), :]], axis=1)

    def keep_pair(index, value):
        for half, part in enumerate(split(value)):
            both[rows(index), half * PAIR : (half + 1) * PAIR] = part

    def regroup_places(group):
        low, cell = [], []
        for member in range(GROUP):
            spots = place_lists[group * GROUP + member, :, :].astype(jnp.int32)
            low.append((spots // 64 % 32).astype(F32))
            cell.append((spots // 2048 * 64 + spots % 64).astype(F32))
        for part in range(4):
            low_parts[group, part, :, :] = regroup(low, part)
            cell_parts[group, part, :, :] = regroup(cell, part)

    def regroup_values(group, chunk):
        span = slice(chunk * tall, (chunk + 1) * tall)
        members = [value_lists[group * GROUP + member, span, :] for member in range(GROUP)]
        for part in range(4):
            value_parts[group, part, span, :] = regroup(members, part)

    loop(replicas - 1, lambda step: place_copy(step, source(step)).wait_recv())
    spans = 4 * quads
    count_cell, count_low = counting(PAIR, GROUP * 32), counting(32, GROUP * 32)

    def cells(group, span):
        return pl.ds(pl.multiple_of((group * spans + span) * PAIR, PAIR), PAIR)

    def mark(group):
        regroup_places(group)
        for span in range(spans):
            cell = cell_parts[group, span % 4, pl.ds(line(span // 4), 1), :]
            hots[cells(group, span), :] = flat(
                jnp.where(count_cell == spread(cell), one, zero)
            ).astype(F8)

    def decode(group, span):
        place = pl.ds(line(span // 4), 1)
        here = count_low == spread(low_parts[group, span % 4, place, :])
        halves = split(jnp.broadcast_to(value_parts[group, span % 4, place, :], (16, GROUP * 32)))
        left = jnp.concatenate([flat(jnp.where(here, half[None], zero)) for half in halves], axis=0)
        result = dot_t(left, hots[cells(group, span), :])
        return result[:32, :] + result[32:, :]

    each(groups, mark)

    square = jnp.zeros((8, PAIR), F32)
    for chunk in range(chunks):
        loop(replicas - 1, lambda step: value_copy(chunk, step, source(step)).wait_recv())
        each(groups, lambda group: regroup_values(group, chunk))
        for span in range(chunk * per * 4, (chunk + 1) * per * 4):
            total = decode(0, span)
            if groups > 1:
                total = lax.fori_loop(1, groups, lambda step, acc: acc + decode(step, span), total)
            square = square + jnp.sum((total * total).reshape(4, 8, PAIR), axis=0)
            sums[pl.ds(span * 32, 32), :] = total

    squares[mine, :, :] = square

    def square_copy(step, slot):
        return pltpu.make_async_remote_copy(
            src_ref=squares.at[slot], dst_ref=squares.at[slot],
            send_sem=square_send.at[step], recv_sem=square_recv.at[slot],
            device_id={"mp": other_part(step)},
            device_id_type=pl.DeviceIdType.MESH,
        )

    loop(parts - 1, lambda step: square_copy(step, mine).start())

    for load in loads[2:4]:
        load.wait()
    first = lane_part((32, PAIR)) < 2
    for pair in range(2 * quads):
        left, right = (sums[pl.ds((2 * pair + side) * 32, 32), :] for side in range(2))
        top = jnp.where(first, left, pltpu.roll(right, 64, axis=1))
        bottom = jnp.where(first, pltpu.roll(left, 64, axis=1), right)
        keep_pair(pair, jnp.concatenate([top, bottom], axis=0))
    coefs[...] = column_transform(both[...], columns_ref[...])
    for index in range(quads):
        update[:, block(index)] = row_transform(rows_ref[...], quad(coefs, index))
    for index in range(quads):
        scaled = row_side[rows(index), :] * value_lists[me, pl.ds(line(index), 1), :]
        high, low = split(scaled)
        left = jnp.concatenate(
            [jnp.concatenate([high, high], axis=1), jnp.concatenate([low, low], axis=1)], axis=0
        )
        back = dot_t(left, column_side[block(index), :])
        summed[:, block(index)] = summed[:, block(index)] - (back[:64, :] + back[64:, :])

    loads[4].wait()
    loop(replicas - 1, lambda step: place_copy(step, me).wait_send())
    for chunk in range(chunks):
        loop(replicas - 1, lambda step: value_copy(chunk, step, me).wait_send())
    loop(parts - 1, lambda step: square_copy(step, mine).wait_send())
    loop(
        parts - 1,
        lambda step: square_copy(step, part_source(step)).wait_recv(),
    )


def deliver(chunks, entries, summed, update, weights, squares, out_momentum_ref, out_weights_ref, result, out_sem):
    share = weights.shape[1] // chunks
    first = pltpu.make_async_copy(summed, out_momentum_ref.at[0], out_sem.at[chunks])
    first.start()
    meansq = jnp.sum(jnp.sum(squares[...], axis=0)) / entries
    factor = lax.rsqrt(jnp.full((1, share), meansq + 1.0, F32))
    stores = []
    for chunk in range(chunks):
        span = pl.ds(chunk * share, share)
        result[:, span] = weights[:, span] - update[:, span] * factor
        stores.append(pltpu.make_async_copy(result.at[:, span], out_weights_ref.at[:, span], out_sem.at[chunk]))
        stores[-1].start()
    first.wait()
    for store in stores:
        store.wait()


def local(replicas, parts, gradient, momentum, weights, positions):
    height, width = weights.shape
    quads = width // QUAD
    tables = side_tables()
    anywhere = pl.BlockSpec(memory_space=pl.ANY)
    vmem = pl.BlockSpec(memory_space=pltpu.VMEM)
    chunks = CHUNKS if quads % CHUNKS == 0 else 1
    listed = chunks * (-(-(quads // chunks) // 8) * 8)
    groups = -(-replicas // GROUP)
    entries = positions.shape[-1]
    wide = jax.ShapeDtypeStruct(weights.shape, F32)
    results = pl.pallas_call(
        functools.partial(kernel, replicas, parts, chunks),
        out_shape=(wide, wide, wide, jax.ShapeDtypeStruct((parts, 8, PAIR), F32)),
        in_specs=[pl.BlockSpec(memory_space=pltpu.HBM)] * 7,
        out_specs=(vmem,) * 4,
        scratch_shapes=[
            pltpu.VMEM((height, width), BF16),
            pltpu.VMEM((height, width), F32),
            pltpu.VMEM((entries, 4 * quads), jnp.int32),
            *[pltpu.VMEM(table.shape, BF16) for table in tables],
            pltpu.VMEM((4 * quads, entries), jnp.int32),
            pltpu.VMEM((quads * 64, PAIR), F32),
            pltpu.VMEM((quads * QUAD, QUAD), BF16),
            pltpu.VMEM((2 * quads * 64, QUAD), BF16),
            pltpu.VMEM((2 * quads * 64, PAIR), F32),
            pltpu.VMEM((groups * GROUP, listed, PAIR), F32),
            pltpu.VMEM((groups * GROUP, listed, PAIR), F32),
            pltpu.VMEM((groups, 4, listed, GROUP * 32), F32),
            pltpu.VMEM((groups, 4, listed, GROUP * 32), F32),
            pltpu.VMEM((groups, 4, listed, GROUP * 32), F32),
            pltpu.VMEM((groups * 4 * quads * PAIR, GROUP * 32), F8),
            pltpu.VMEM((4 * quads * 32, PAIR), F32),
            pltpu.SemaphoreType.DMA((5,)),
            pltpu.SemaphoreType.DMA((chunks, 2)),
            pltpu.SemaphoreType.DMA((replicas,)),
            pltpu.SemaphoreType.DMA((replicas,)),
            pltpu.SemaphoreType.DMA((chunks, replicas)),
            pltpu.SemaphoreType.DMA((chunks, replicas)),
            pltpu.SemaphoreType.DMA((parts,)),
            pltpu.SemaphoreType.DMA((parts,)),
        ],
        compiler_params=pltpu.CompilerParams(
            collective_id=0, has_side_effects=True, vmem_limit_bytes=(22 + 2 * groups) * 1024 * 1024
        ),
    )(
        *(
            pltpu.with_memory_space_constraint(array, pltpu.HBM)
            for array in (
                gradient, momentum, weights, jnp.swapaxes(positions, 2, 3), *map(jnp.asarray, tables),
            )
        )
    )
    return pl.pallas_call(
        functools.partial(deliver, chunks, float(height * width * parts)),
        out_shape=(
            jax.ShapeDtypeStruct(momentum.shape, F32),
            jax.ShapeDtypeStruct(weights.shape, F32),
        ),
        in_specs=[vmem] * 4,
        out_specs=(anywhere, anywhere),
        scratch_shapes=[pltpu.VMEM((height, width), F32), pltpu.SemaphoreType.DMA((chunks + 1,))],
        compiler_params=pltpu.CompilerParams(vmem_limit_bytes=8 * 1024 * 1024),
    )(*results)


def solution(mesh):
    placed = (P("dp", None, "mp"), P("dp", None, "mp"), P(None, "mp"), P("dp", None, "mp", None))
    return jax.shard_map(
        functools.partial(local, mesh.shape["dp"], mesh.shape["mp"]),
        mesh=mesh,
        in_specs=placed,
        out_specs=(P("dp", None, "mp"), P(None, "mp")),
        check_vma=False,
    )
```

```python
import functools

import jax
import jax.numpy as jnp
import numpy as np
from jax import lax
from jax.experimental import pallas as pl
from jax.experimental.pallas import tpu as pltpu
from jax.sharding import PartitionSpec as P

QUAD = 256
PAIR = 128
GROUP = 8
CHUNKS = 1
F32 = jnp.float32
BF16 = jnp.bfloat16
F8 = jnp.float8_e4m3fn


def dct_table():
    column = np.arange(64, dtype=np.float64)
    freq = column[:, None]
    factor = np.where(freq == 0, np.sqrt(1.0 / 64), np.sqrt(2.0 / 64))
    return factor * np.cos(np.pi * (2.0 * column[None, :] + 1.0) * freq / 128.0)


def halves(table):
    high = np.asarray(table, np.float32).astype(jnp.bfloat16)
    low = np.asarray(table - high.astype(np.float64), np.float32).astype(jnp.bfloat16)
    return high, low


def side_tables():
    table = dct_table()
    high, low = halves(table.T)
    gather = np.concatenate([high, low], axis=1)
    rows = np.concatenate([high, low, high, low], axis=1)
    columns = np.concatenate(halves(np.kron(np.eye(2), table)), axis=1)
    return gather, np.concatenate([rows, columns], axis=0)


def split(value):
    high = value.astype(BF16)
    return high, (value - high.astype(F32)).astype(BF16)


def dot(a, b):
    return jnp.dot(a, b, preferred_element_type=F32)


def dot_t(a, b):
    return lax.dot_general(a, b, (((1,), (1,)), ((), ())), preferred_element_type=F32)


def row_transform(table, value):
    high, low = split(value)
    return dot(table, jnp.concatenate([high, high, low, low], axis=0))


def column_transform(both, table):
    result = dot(both, jnp.concatenate([table, table], axis=0))
    return result[:, :PAIR] + result[:, PAIR:]


def counting(rows, lanes):
    count = lax.broadcasted_iota(jnp.int32, (rows, lanes), 0).astype(F32)
    return count.astype(BF16).reshape(-1, 16, lanes)


def spread(row):
    return jnp.broadcast_to(row, (16, row.shape[1])).astype(BF16)[None]


def flat(tiles):
    return tiles.reshape(-1, tiles.shape[-1])


def frequencies(places):
    return (places // 64).astype(F32), (places % 64).astype(F32)


def lane_part(shape):
    return lax.broadcasted_iota(jnp.int32, shape, 1) // 32


def regroup(members, part):
    result = []
    for start in range(0, GROUP, 4):
        joined = members[start + -part % 4]
        for place in range(1, 4):
            member = members[start + (place - part) % 4]
            joined = jnp.where(lane_part(joined.shape) == place, member, joined)
        result.append(joined)
    return jnp.concatenate(result, axis=1)


def partner(me, count, step):
    return step + (step - me + count) // count


def loop(count, body):
    if count <= 16:
        for step in range(count):
            body(step)
    else:
        lax.fori_loop(0, count, lambda step, carry: (body(step), carry)[1], 0)


def each(count, body):
    if count == 1:
        body(0)
    else:
        lax.fori_loop(0, count, lambda step, carry: (body(step), carry)[1], 0)


def kernel(
    replicas, parts, chunks,
    gradient_ref, momentum_ref, weights_ref, places_hbm, gather_hbm, tables_hbm,
    summed, update, wts, squares,
    grad, mom, places_ref, gather_ref, tables_ref, flipped, row_side, column_side, both, coefs,
    place_lists, value_lists, low_parts, cell_parts, value_parts, hots, sums,
    in_sem, chunk_sem, place_sem, value_sem, square_sem,
):
    me, mine = lax.axis_index("dp"), lax.axis_index("mp")
    width = summed.shape[1]
    quads = width // QUAD
    per = quads // chunks
    tall = place_lists.shape[1] // chunks

    def block(index):
        return pl.ds(index * QUAD, QUAD)

    def rows(index):
        return pl.ds(index * 64, 64)

    def line(index):
        return index // per * tall + index % per

    def chunk_loads(chunk):
        span = pl.ds(chunk * per * QUAD, per * QUAD)
        return [
            pltpu.make_async_copy(source.at[0, :, span], target.at[:, span], chunk_sem.at[chunk, index])
            for index, (source, target) in enumerate(((gradient_ref, grad), (momentum_ref, mom)))
        ]

    loads = [
        pltpu.make_async_copy(source, target, in_sem.at[index])
        for index, (source, target) in enumerate(
            (
                (places_hbm.at[0, 0], places_ref), (gather_hbm, gather_ref),
                (tables_hbm, tables_ref), (weights_ref, wts),
            )
        )
    ]
    for load in loads[:2]:
        load.start()
    for chunk in range(chunks):
        for load in chunk_loads(chunk):
            load.start()

    barrier = pltpu.get_barrier_semaphore()
    replica = functools.partial(partner, me, replicas)
    other_part = functools.partial(partner, mine, parts)

    def greet_replica(step):
        pl.semaphore_signal(
            barrier, inc=1, device_id={"dp": replica(step)},
            device_id_type=pl.DeviceIdType.MESH,
        )

    def greet_part(step):
        pl.semaphore_signal(
            barrier, inc=1, device_id={"mp": other_part(step)},
            device_id_type=pl.DeviceIdType.MESH,
        )

    loop(replicas - 1, greet_replica)
    loop(parts - 1, greet_part)

    def list_copy(lists, sems, step, slot, span):
        return pltpu.make_async_remote_copy(
            src_ref=lists.at[slot, span], dst_ref=lists.at[slot, span],
            send_sem=sems.at[0], recv_sem=sems.at[1],
            device_id={"dp": replica(step)}, device_id_type=pl.DeviceIdType.MESH,
        )

    def place_copy(step, slot):
        return list_copy(place_lists, place_sem, step, slot, pl.ds(0, (chunks - 1) * tall + per))

    def value_copy(chunk, step, slot):
        return list_copy(value_lists, value_sem.at[chunk], step, slot, pl.ds(chunk * tall, per))

    others = pl.ds(0, replicas - 1)

    groups = place_lists.shape[0] // GROUP
    for slot in range(replicas, groups * GROUP):
        place_lists[slot, :, :] = jnp.zeros(place_lists.shape[1:], F32)
        value_lists[slot, :, :] = jnp.zeros(value_lists.shape[1:], F32)

    loads[0].wait()
    flipped[...] = jnp.transpose(places_ref[...])
    turn = lax.rem(me, 4)
    places = jnp.concatenate(
        [flipped[pl.ds(lax.rem(place + 4 - turn, 4), quads, stride=4), :] for place in range(4)], axis=1
    )
    for chunk in range(chunks):
        place_lists[me, chunk * tall : chunk * tall + per, :] = places[
            chunk * per : (chunk + 1) * per
        ].astype(F32)

    zero, one = jnp.zeros((), BF16), jnp.ones((), BF16)
    count = counting(64, PAIR)
    row_freqs, column_freqs = frequencies(places)
    lanes = lax.rem(lane_part((64, PAIR)) + 4 - turn, 4)

    def hot(row):
        return flat(jnp.where(count == spread(row), one, zero))

    loads[1].wait()
    for index in range(quads):
        pair = [hot(freqs[index : index + 1, :]) for freqs in (row_freqs, column_freqs)]
        both_hot = jnp.concatenate(pair, axis=1)
        found = dot(gather_ref[...], jnp.concatenate([both_hot, both_hot], axis=0))
        row_side[rows(index), :] = found[:, :PAIR]
        for half, side in enumerate(split(found[:, PAIR:])):
            for part in range(4):
                column_side[pl.ds(index * QUAD + part * 64, 64), half * PAIR : (half + 1) * PAIR] = (
                    jnp.where(lanes == part, side, zero)
                )

    pl.semaphore_wait(barrier, replicas - 1 + parts - 1)
    loop(replicas - 1, lambda step: place_copy(step, me).start())

    for chunk in range(chunks):
        for load in chunk_loads(chunk):
            load.wait()
        for index in range(chunk * per, (chunk + 1) * per):
            value = 0.9 * mom[:, block(index)] + grad[:, block(index)].astype(F32)
            summed[:, block(index)] = value
            found = dot(jnp.concatenate(split(value), axis=0), column_side[block(index), :])
            found = found[:64, :] + found[64:, :]
            found = (found[:, :PAIR] + found[:, PAIR:]) * row_side[rows(index), :]
            value_lists[me, pl.ds(line(index), 1), :] = jnp.sum(found, axis=0, keepdims=True)
        loop(replicas - 1, lambda step: value_copy(chunk, step, me).start())
    for load in loads[2:]:
        load.start()

    def quad(ref, index):
        return jnp.concatenate([ref[rows(2 * index), :], ref[rows(2 * index + 1), :]], axis=1)

    def keep_pair(index, value):
        for half, part in enumerate(split(value)):
            both[rows(index), half * PAIR : (half + 1) * PAIR] = part

    def regroup_places(group):
        low, cell = [], []
        for member in range(GROUP):
            spots = place_lists[group * GROUP + member, :, :].astype(jnp.int32)
            low.append((spots // 64 % 32).astype(F32))
            cell.append((spots // 2048 * 64 + spots % 64).astype(F32))
        for part in range(4):
            low_parts[group, part, :, :] = regroup(low, part)
            cell_parts[group, part, :, :] = regroup(cell, part)

    def regroup_values(group, chunk):
        span = slice(chunk * tall, (chunk + 1) * tall)
        members = [value_lists[group * GROUP + member, span, :] for member in range(GROUP)]
        for part in range(4):
            value_parts[group, part, span, :] = regroup(members, part)

    place_copy(0, others).wait_recv()
    spans = 4 * quads
    count_cell, count_low = counting(PAIR, GROUP * 32), counting(32, GROUP * 32)

    def cells(group, span):
        return pl.ds(pl.multiple_of((group * spans + span) * PAIR, PAIR), PAIR)

    def mark(group):
        regroup_places(group)
        for span in range(spans):
            cell = cell_parts[group, span % 4, pl.ds(line(span // 4), 1), :]
            hots[cells(group, span), :] = flat(
                jnp.where(count_cell == spread(cell), one, zero)
            ).astype(F8)

    def decode(group, span):
        place = pl.ds(line(span // 4), 1)
        here = count_low == spread(low_parts[group, span % 4, place, :])
        halves = split(jnp.broadcast_to(value_parts[group, span % 4, place, :], (16, GROUP * 32)))
        left = jnp.concatenate([flat(jnp.where(here, half[None], zero)) for half in halves], axis=0)
        result = dot_t(left, hots[cells(group, span), :])
        return result[:32, :] + result[32:, :]

    each(groups, mark)

    square = jnp.zeros((8, PAIR), F32)
    for chunk in range(chunks):
        value_copy(chunk, 0, others).wait_recv()
        each(groups, lambda group: regroup_values(group, chunk))
        for span in range(chunk * per * 4, (chunk + 1) * per * 4):
            total = decode(0, span)
            if groups > 1:
                total = lax.fori_loop(1, groups, lambda step, acc: acc + decode(step, span), total)
            square = square + jnp.sum((total * total).reshape(4, 8, PAIR), axis=0)
            sums[pl.ds(span * 32, 32), :] = total

    squares[mine, 0:1, :] = jnp.sum(square, axis=0, keepdims=True)

    def square_copy(step, slot):
        return pltpu.make_async_remote_copy(
            src_ref=squares.at[slot, pl.ds(0, 1)], dst_ref=squares.at[slot, pl.ds(0, 1)],
            send_sem=square_sem.at[0], recv_sem=square_sem.at[1],
            device_id={"mp": other_part(step)}, device_id_type=pl.DeviceIdType.MESH,
        )

    loop(parts - 1, lambda step: square_copy(step, mine).start())

    loads[2].wait()
    first = lane_part((32, PAIR)) < 2
    for pair in range(2 * quads):
        left, right = (sums[pl.ds((2 * pair + side) * 32, 32), :] for side in range(2))
        top = jnp.where(first, left, pltpu.roll(right, 64, axis=1))
        bottom = jnp.where(first, pltpu.roll(left, 64, axis=1), right)
        keep_pair(pair, jnp.concatenate([top, bottom], axis=0))
    coefs[...] = column_transform(both[...], tables_ref[64:, :])
    for index in range(quads):
        update[:, block(index)] = row_transform(tables_ref[:64, :], quad(coefs, index))
    for index in range(quads):
        scaled = row_side[rows(index), :] * value_lists[me, pl.ds(line(index), 1), :]
        high, low = split(scaled)
        left = jnp.concatenate(
            [jnp.concatenate([high, high], axis=1), jnp.concatenate([low, low], axis=1)], axis=0
        )
        back = dot_t(left, column_side[block(index), :])
        summed[:, block(index)] = summed[:, block(index)] - (back[:64, :] + back[64:, :])

    loads[3].wait()
    place_copy(0, others).wait_send()
    for chunk in range(chunks):
        value_copy(chunk, 0, others).wait_send()
    square_copy(0, pl.ds(0, parts - 1)).wait()


def deliver(chunks, entries, summed, update, weights, squares, out_momentum_ref, out_weights_ref, result, out_sem):
    share = weights.shape[1] // chunks
    first = pltpu.make_async_copy(summed, out_momentum_ref.at[0], out_sem.at[chunks])
    first.start()
    meansq = jnp.sum(squares[:, 0, :]) / entries
    factor = lax.rsqrt(jnp.full((1, share), meansq + 1.0, F32))
    stores = []
    for chunk in range(chunks):
        span = pl.ds(chunk * share, share)
        result[:, span] = weights[:, span] - update[:, span] * factor
        stores.append(pltpu.make_async_copy(result.at[:, span], out_weights_ref.at[:, span], out_sem.at[chunk]))
        stores[-1].start()
    first.wait()
    for store in stores:
        store.wait()


def local(replicas, parts, gradient, momentum, weights, positions):
    height, width = weights.shape
    quads = width // QUAD
    tables = side_tables()
    anywhere = pl.BlockSpec(memory_space=pl.ANY)
    vmem = pl.BlockSpec(memory_space=pltpu.VMEM)
    chunks = CHUNKS if quads % CHUNKS == 0 else 1
    listed = chunks * (-(-(quads // chunks) // 8) * 8)
    groups = -(-replicas // GROUP)
    entries = positions.shape[-1]
    wide = jax.ShapeDtypeStruct(weights.shape, F32)
    results = pl.pallas_call(
        functools.partial(kernel, replicas, parts, chunks),
        out_shape=(wide, wide, wide, jax.ShapeDtypeStruct((parts, 8, PAIR), F32)),
        in_specs=[pl.BlockSpec(memory_space=pltpu.HBM)] * 6,
        out_specs=(vmem,) * 4,
        scratch_shapes=[
            pltpu.VMEM((height, width), BF16),
            pltpu.VMEM((height, width), F32),
            pltpu.VMEM((entries, 4 * quads), jnp.int32),
            *[pltpu.VMEM(table.shape, BF16) for table in tables],
            pltpu.VMEM((4 * quads, entries), jnp.int32),
            pltpu.VMEM((quads * 64, PAIR), F32),
            pltpu.VMEM((quads * QUAD, QUAD), BF16),
            pltpu.VMEM((2 * quads * 64, QUAD), BF16),
            pltpu.VMEM((2 * quads * 64, PAIR), F32),
            pltpu.VMEM((groups * GROUP, listed, PAIR), F32),
            pltpu.VMEM((groups * GROUP, listed, PAIR), F32),
            pltpu.VMEM((groups, 4, listed, GROUP * 32), F32),
            pltpu.VMEM((groups, 4, listed, GROUP * 32), F32),
            pltpu.VMEM((groups, 4, listed, GROUP * 32), F32),
            pltpu.VMEM((groups * 4 * quads * PAIR, GROUP * 32), F8),
            pltpu.VMEM((4 * quads * 32, PAIR), F32),
            pltpu.SemaphoreType.DMA((4,)),
            pltpu.SemaphoreType.DMA((chunks, 2)),
            pltpu.SemaphoreType.DMA((2,)),
            pltpu.SemaphoreType.DMA((chunks, 2)),
            pltpu.SemaphoreType.DMA((2,)),
        ],
        compiler_params=pltpu.CompilerParams(
            collective_id=0, has_side_effects=True, vmem_limit_bytes=(22 + 2 * groups) * 1024 * 1024
        ),
    )(
        *(
            pltpu.with_memory_space_constraint(array, pltpu.HBM)
            for array in (
                gradient, momentum, weights, jnp.swapaxes(positions, 2, 3), *map(jnp.asarray, tables),
            )
        )
    )
    return pl.pallas_call(
        functools.partial(deliver, chunks, float(height * width * parts)),
        out_shape=(
            jax.ShapeDtypeStruct(momentum.shape, F32),
            jax.ShapeDtypeStruct(weights.shape, F32),
        ),
        in_specs=[vmem] * 4,
        out_specs=(anywhere, anywhere),
        scratch_shapes=[pltpu.VMEM((height, width), F32), pltpu.SemaphoreType.DMA((chunks + 1,))],
        compiler_params=pltpu.CompilerParams(vmem_limit_bytes=8 * 1024 * 1024),
    )(*results)


def solution(mesh):
    placed = (P("dp", None, "mp"), P("dp", None, "mp"), P(None, "mp"), P("dp", None, "mp", None))
    return jax.shard_map(
        functools.partial(local, mesh.shape["dp"], mesh.shape["mp"]),
        mesh=mesh,
        in_specs=placed,
        out_specs=(P("dp", None, "mp"), P(None, "mp")),
        check_vma=False,
    )
```

```python
import functools

import jax
import jax.numpy as jnp
import numpy as np
from jax import lax
from jax.experimental import pallas as pl
from jax.experimental.pallas import tpu as pltpu
from jax.sharding import PartitionSpec as P

QUAD = 256
PAIR = 128
GROUP = 8
CHUNKS = 1
F32 = jnp.float32
BF16 = jnp.bfloat16
F8 = jnp.float8_e4m3fn


def dct_table():
    column = np.arange(64, dtype=np.float64)
    freq = column[:, None]
    factor = np.where(freq == 0, np.sqrt(1.0 / 64), np.sqrt(2.0 / 64))
    return factor * np.cos(np.pi * (2.0 * column[None, :] + 1.0) * freq / 128.0)


def halves(table):
    high = np.asarray(table, np.float32).astype(jnp.bfloat16)
    low = np.asarray(table - high.astype(np.float64), np.float32).astype(jnp.bfloat16)
    return high, low


def side_tables():
    table = dct_table()
    high, low = halves(table.T)
    gather = np.concatenate([high, low], axis=1)
    rows = np.concatenate([high, low, high, low], axis=1)
    columns = np.concatenate(halves(np.kron(np.eye(2), table)), axis=1)
    return gather, np.concatenate([rows, columns], axis=0)


def split(value):
    high = value.astype(BF16)
    return high, (value - high.astype(F32)).astype(BF16)


def dot(a, b):
    return jnp.dot(a, b, preferred_element_type=F32)


def dot_t(a, b):
    return lax.dot_general(a, b, (((1,), (1,)), ((), ())), preferred_element_type=F32)


def row_transform(table, value):
    high, low = split(value)
    return dot(table, jnp.concatenate([high, high, low, low], axis=0))


def column_transform(both, table):
    result = dot(both, jnp.concatenate([table, table], axis=0))
    return result[:, :PAIR] + result[:, PAIR:]


def counting(rows, lanes):
    count = lax.broadcasted_iota(jnp.int32, (rows, lanes), 0).astype(F32)
    return count.astype(BF16).reshape(-1, 16, lanes)


def spread(row):
    return jnp.broadcast_to(row, (16, row.shape[1])).astype(BF16)[None]


def flat(tiles):
    return tiles.reshape(-1, tiles.shape[-1])


def frequencies(places):
    return (places // 64).astype(F32), (places % 64).astype(F32)


def lane_part(shape):
    return lax.broadcasted_iota(jnp.int32, shape, 1) // 32


def regroup(members, part):
    result = []
    for start in range(0, GROUP, 4):
        joined = members[start + -part % 4]
        for place in range(1, 4):
            member = members[start + (place - part) % 4]
            joined = jnp.where(lane_part(joined.shape) == place, member, joined)
        result.append(joined)
    return jnp.concatenate(result, axis=1)


def partner(me, count, step):
    return step + (step - me + count) // count


def loop(count, body):
    if count <= 16:
        for step in range(count):
            body(step)
    else:
        lax.fori_loop(0, count, lambda step, carry: (body(step), carry)[1], 0)


def each(count, body):
    if count == 1:
        body(0)
    else:
        lax.fori_loop(0, count, lambda step, carry: (body(step), carry)[1], 0)


def kernel(
    replicas, parts, chunks,
    gradient_ref, momentum_ref, weights_ref, places_hbm, gather_hbm, tables_hbm,
    summed, update, wts, squares,
    grad, mom, places_ref, gather_ref, tables_ref, flipped, row_side, column_high, column_low, both, coefs,
    place_lists, value_lists, low_parts, cell_parts, value_parts, hots, sums,
    in_sem, chunk_sem, place_sem, value_sem, square_sem,
):
    me, mine = lax.axis_index("dp"), lax.axis_index("mp")
    width = summed.shape[1]
    quads = width // QUAD
    per = quads // chunks
    tall = place_lists.shape[1] // chunks

    def block(index):
        return pl.ds(index * QUAD, QUAD)

    def rows(index):
        return pl.ds(index * 64, 64)

    def line(index):
        return index // per * tall + index % per

    def chunk_loads(chunk):
        span = pl.ds(chunk * per * QUAD, per * QUAD)
        return [
            pltpu.make_async_copy(source.at[0, :, span], target.at[:, span], chunk_sem.at[chunk, index])
            for index, (source, target) in enumerate(((gradient_ref, grad), (momentum_ref, mom)))
        ]

    loads = [
        pltpu.make_async_copy(source, target, in_sem.at[index])
        for index, (source, target) in enumerate(
            (
                (places_hbm.at[0, 0], places_ref), (gather_hbm, gather_ref),
                (tables_hbm, tables_ref), (weights_ref, wts),
            )
        )
    ]
    for load in loads[:2]:
        load.start()
    for chunk in range(chunks):
        for load in chunk_loads(chunk):
            load.start()

    barrier = pltpu.get_barrier_semaphore()
    replica = functools.partial(partner, me, replicas)
    other_part = functools.partial(partner, mine, parts)

    def greet_replica(step):
        pl.semaphore_signal(
            barrier, inc=1, device_id={"dp": replica(step)},
            device_id_type=pl.DeviceIdType.MESH,
        )

    def greet_part(step):
        pl.semaphore_signal(
            barrier, inc=1, device_id={"mp": other_part(step)},
            device_id_type=pl.DeviceIdType.MESH,
        )

    loop(replicas - 1, lambda step: greet_replica(replicas - 2 - step))
    loop(parts - 1, greet_part)

    def list_copy(lists, sems, step, slot, span):
        return pltpu.make_async_remote_copy(
            src_ref=lists.at[slot, span], dst_ref=lists.at[slot, span],
            send_sem=sems.at[0], recv_sem=sems.at[1],
            device_id={"dp": replica(step)}, device_id_type=pl.DeviceIdType.MESH,
        )

    def place_copy(step, slot):
        return list_copy(place_lists, place_sem, step, slot, pl.ds(0, (chunks - 1) * tall + per))

    def value_copy(chunk, step, slot):
        return list_copy(value_lists, value_sem.at[chunk], step, slot, pl.ds(chunk * tall, per))

    others = pl.ds(0, replicas - 1)

    groups = place_lists.shape[0] // GROUP
    for slot in range(replicas, groups * GROUP):
        place_lists[slot, :, :] = jnp.zeros(place_lists.shape[1:], F32)
        value_lists[slot, :, :] = jnp.zeros(value_lists.shape[1:], F32)

    loads[0].wait()
    flipped[...] = jnp.transpose(places_ref[...])
    turn = lax.rem(me, 4)
    places = jnp.concatenate(
        [flipped[pl.ds(lax.rem(place + 4 - turn, 4), quads, stride=4), :] for place in range(4)], axis=1
    )
    for chunk in range(chunks):
        place_lists[me, chunk * tall : chunk * tall + per, :] = places[
            chunk * per : (chunk + 1) * per
        ].astype(F32)

    pl.semaphore_wait(barrier, replicas - 1 + parts - 1)
    loop(replicas - 1, lambda step: place_copy(step, me).start())

    zero, one = jnp.zeros((), BF16), jnp.ones((), BF16)
    count = counting(64, PAIR)
    row_freqs, column_freqs = frequencies(places)
    lanes = lax.rem(lane_part((64, QUAD)) + 4 - turn, 4)

    def hot(row):
        return flat(jnp.where(count == spread(row), one, zero))

    def total(index):
        return 0.9 * mom[:, block(index)] + grad[:, block(index)].astype(F32)

    def column_side(index):
        side = jnp.concatenate([column_high[rows(index), :], column_low[rows(index), :]], axis=1)
        return jnp.concatenate([jnp.where(lanes == part, side, zero) for part in range(4)], axis=0)

    loads[1].wait()
    for index in range(quads):
        pair = [hot(freqs[index : index + 1, :]) for freqs in (row_freqs, column_freqs)]
        both_hot = jnp.concatenate(pair, axis=1)
        found = dot(gather_ref[...], jnp.concatenate([both_hot, both_hot], axis=0))
        row_side[rows(index), :] = found[:, :PAIR]
        column_high[rows(index), :], column_low[rows(index), :] = split(found[:, PAIR:])

    for chunk in range(chunks):
        for load in chunk_loads(chunk):
            load.wait()
        for index in range(chunk * per, (chunk + 1) * per):
            found = dot(jnp.concatenate(split(total(index)), axis=0), column_side(index))
            found = found[:64, :] + found[64:, :]
            found = (found[:, :PAIR] + found[:, PAIR:]) * row_side[rows(index), :]
            value_lists[me, pl.ds(line(index), 1), :] = jnp.sum(found, axis=0, keepdims=True)
        loop(replicas - 1, lambda step: value_copy(chunk, step, me).start())
    for load in loads[2:]:
        load.start()

    def quad(ref, index):
        return jnp.concatenate([ref[rows(2 * index), :], ref[rows(2 * index + 1), :]], axis=1)

    def keep_pair(index, value):
        for half, part in enumerate(split(value)):
            both[rows(index), half * PAIR : (half + 1) * PAIR] = part

    def regroup_places(group):
        low, cell = [], []
        for member in range(GROUP):
            spots = place_lists[group * GROUP + member, :, :].astype(jnp.int32)
            low.append((spots // 64 % 32).astype(F32))
            cell.append((spots // 2048 * 64 + spots % 64).astype(F32))
        for part in range(4):
            low_parts[group, part, :, :] = regroup(low, part)
            cell_parts[group, part, :, :] = regroup(cell, part)

    def regroup_values(group, chunk):
        span = slice(chunk * tall, (chunk + 1) * tall)
        members = [value_lists[group * GROUP + member, span, :] for member in range(GROUP)]
        for part in range(4):
            value_parts[group, part, span, :] = regroup(members, part)

    place_copy(0, others).wait_recv()
    spans = 4 * quads
    count_cell, count_low = counting(PAIR, GROUP * 32), counting(32, GROUP * 32)

    def cells(group, span):
        return pl.ds(pl.multiple_of((group * spans + span) * PAIR, PAIR), PAIR)

    def mark(group):
        regroup_places(group)
        for span in range(spans):
            cell = cell_parts[group, span % 4, pl.ds(line(span // 4), 1), :]
            hots[cells(group, span), :] = flat(
                jnp.where(count_cell == spread(cell), one, zero)
            ).astype(F8)

    def decode(group, span):
        place = pl.ds(line(span // 4), 1)
        here = count_low == spread(low_parts[group, span % 4, place, :])
        halves = split(jnp.broadcast_to(value_parts[group, span % 4, place, :], (16, GROUP * 32)))
        left = jnp.concatenate([flat(jnp.where(here, half[None], zero)) for half in halves], axis=0)
        result = dot_t(left, hots[cells(group, span), :])
        return result[:32, :] + result[32:, :]

    each(groups, mark)

    square = jnp.zeros((8, PAIR), F32)
    for chunk in range(chunks):
        value_copy(chunk, 0, others).wait_recv()
        each(groups, lambda group: regroup_values(group, chunk))
        for span in range(chunk * per * 4, (chunk + 1) * per * 4):
            cells_sum = decode(0, span)
            if groups > 1:
                cells_sum = lax.fori_loop(1, groups, lambda step, acc: acc + decode(step, span), cells_sum)
            square = square + jnp.sum((cells_sum * cells_sum).reshape(4, 8, PAIR), axis=0)
            sums[pl.ds(span * 32, 32), :] = cells_sum

    squares[mine, 0:1, :] = jnp.sum(square, axis=0, keepdims=True)

    def square_copy(step, slot):
        return pltpu.make_async_remote_copy(
            src_ref=squares.at[slot, pl.ds(0, 1)], dst_ref=squares.at[slot, pl.ds(0, 1)],
            send_sem=square_sem.at[0], recv_sem=square_sem.at[1],
            device_id={"mp": other_part(step)}, device_id_type=pl.DeviceIdType.MESH,
        )

    loop(parts - 1, lambda step: square_copy(step, mine).start())

    loads[2].wait()
    first = lane_part((32, PAIR)) < 2
    for pair in range(2 * quads):
        left, right = (sums[pl.ds((2 * pair + side) * 32, 32), :] for side in range(2))
        top = jnp.where(first, left, pltpu.roll(right, 64, axis=1))
        bottom = jnp.where(first, pltpu.roll(left, 64, axis=1), right)
        keep_pair(pair, jnp.concatenate([top, bottom], axis=0))
    coefs[...] = column_transform(both[...], tables_ref[64:, :])
    for index in range(quads):
        update[:, block(index)] = row_transform(tables_ref[:64, :], quad(coefs, index))
    for index in range(quads):
        scaled = row_side[rows(index), :] * value_lists[me, pl.ds(line(index), 1), :]
        high, low = split(scaled)
        left = jnp.concatenate(
            [jnp.concatenate([high, high], axis=1), jnp.concatenate([low, low], axis=1)], axis=0
        )
        back = dot_t(left, column_side(index))
        summed[:, block(index)] = total(index) - (back[:64, :] + back[64:, :])

    loads[3].wait()
    place_copy(0, others).wait_send()
    for chunk in range(chunks):
        value_copy(chunk, 0, others).wait_send()
    square_copy(0, pl.ds(0, parts - 1)).wait()


def deliver(chunks, entries, summed, update, weights, squares, out_momentum_ref, out_weights_ref, result, out_sem):
    share = weights.shape[1] // chunks
    first = pltpu.make_async_copy(summed, out_momentum_ref.at[0], out_sem.at[chunks])
    first.start()
    meansq = jnp.sum(squares[:, 0, :]) / entries
    factor = lax.rsqrt(jnp.full((1, share), meansq + 1.0, F32))
    stores = []
    for chunk in range(chunks):
        span = pl.ds(chunk * share, share)
        result[:, span] = weights[:, span] - update[:, span] * factor
        stores.append(pltpu.make_async_copy(result.at[:, span], out_weights_ref.at[:, span], out_sem.at[chunk]))
        stores[-1].start()
    first.wait()
    for store in stores:
        store.wait()


def local(replicas, parts, gradient, momentum, weights, positions):
    height, width = weights.shape
    quads = width // QUAD
    tables = side_tables()
    anywhere = pl.BlockSpec(memory_space=pl.ANY)
    vmem = pl.BlockSpec(memory_space=pltpu.VMEM)
    chunks = CHUNKS if quads % CHUNKS == 0 else 1
    listed = chunks * (-(-(quads // chunks) // 8) * 8)
    groups = -(-replicas // GROUP)
    entries = positions.shape[-1]
    wide = jax.ShapeDtypeStruct(weights.shape, F32)
    results = pl.pallas_call(
        functools.partial(kernel, replicas, parts, chunks),
        out_shape=(wide, wide, wide, jax.ShapeDtypeStruct((parts, 8, PAIR), F32)),
        in_specs=[pl.BlockSpec(memory_space=pltpu.HBM)] * 6,
        out_specs=(vmem,) * 4,
        scratch_shapes=[
            pltpu.VMEM((height, width), BF16),
            pltpu.VMEM((height, width), F32),
            pltpu.VMEM((entries, 4 * quads), jnp.int32),
            *[pltpu.VMEM(table.shape, BF16) for table in tables],
            pltpu.VMEM((4 * quads, entries), jnp.int32),
            pltpu.VMEM((quads * 64, PAIR), F32),
            pltpu.VMEM((quads * 64, PAIR), BF16),
            pltpu.VMEM((quads * 64, PAIR), BF16),
            pltpu.VMEM((2 * quads * 64, QUAD), BF16),
            pltpu.VMEM((2 * quads * 64, PAIR), F32),
            pltpu.VMEM((groups * GROUP, listed, PAIR), F32),
            pltpu.VMEM((groups * GROUP, listed, PAIR), F32),
            pltpu.VMEM((groups, 4, listed, GROUP * 32), F32),
            pltpu.VMEM((groups, 4, listed, GROUP * 32), F32),
            pltpu.VMEM((groups, 4, listed, GROUP * 32), F32),
            pltpu.VMEM((groups * 4 * quads * PAIR, GROUP * 32), F8),
            pltpu.VMEM((4 * quads * 32, PAIR), F32),
            pltpu.SemaphoreType.DMA((4,)),
            pltpu.SemaphoreType.DMA((chunks, 2)),
            pltpu.SemaphoreType.DMA((2,)),
            pltpu.SemaphoreType.DMA((chunks, 2)),
            pltpu.SemaphoreType.DMA((2,)),
        ],
        compiler_params=pltpu.CompilerParams(
            collective_id=0, has_side_effects=True, vmem_limit_bytes=(22 + 2 * groups) * 1024 * 1024
        ),
    )(
        *(
            pltpu.with_memory_space_constraint(array, pltpu.HBM)
            for array in (
                gradient, momentum, weights, jnp.swapaxes(positions, 2, 3), *map(jnp.asarray, tables),
            )
        )
    )
    return pl.pallas_call(
        functools.partial(deliver, chunks, float(height * width * parts)),
        out_shape=(
            jax.ShapeDtypeStruct(momentum.shape, F32),
            jax.ShapeDtypeStruct(weights.shape, F32),
        ),
        in_specs=[vmem] * 4,
        out_specs=(anywhere, anywhere),
        scratch_shapes=[pltpu.VMEM((height, width), F32), pltpu.SemaphoreType.DMA((chunks + 1,))],
        compiler_params=pltpu.CompilerParams(vmem_limit_bytes=8 * 1024 * 1024),
    )(*results)


def solution(mesh):
    placed = (P("dp", None, "mp"), P("dp", None, "mp"), P(None, "mp"), P("dp", None, "mp", None))
    return jax.shard_map(
        functools.partial(local, mesh.shape["dp"], mesh.shape["mp"]),
        mesh=mesh,
        in_specs=placed,
        out_specs=(P("dp", None, "mp"), P(None, "mp")),
        check_vma=False,
    )
```

```python
import functools

import jax
import jax.numpy as jnp
import numpy as np
from jax import lax
from jax.experimental import pallas as pl
from jax.experimental.pallas import tpu as pltpu
from jax.sharding import PartitionSpec as P

QUAD = 256
PAIR = 128
GROUP = 8
CHUNKS = 1
EARLY = 1
F32 = jnp.float32
BF16 = jnp.bfloat16
F8 = jnp.float8_e4m3fn


def dct_table():
    column = np.arange(64, dtype=np.float64)
    freq = column[:, None]
    factor = np.where(freq == 0, np.sqrt(1.0 / 64), np.sqrt(2.0 / 64))
    return factor * np.cos(np.pi * (2.0 * column[None, :] + 1.0) * freq / 128.0)


def halves(table):
    high = np.asarray(table, np.float32).astype(jnp.bfloat16)
    low = np.asarray(table - high.astype(np.float64), np.float32).astype(jnp.bfloat16)
    return high, low


def side_tables():
    table = dct_table()
    high, low = halves(table.T)
    gather = np.concatenate([high, low], axis=1)
    rows = np.concatenate([high, low, high, low], axis=1)
    columns = np.concatenate(halves(np.kron(np.eye(2), table)), axis=1)
    return gather, np.concatenate([rows, columns], axis=0)


def split(value):
    high = value.astype(BF16)
    return high, (value - high.astype(F32)).astype(BF16)


def dot(a, b):
    return jnp.dot(a, b, preferred_element_type=F32)


def dot_t(a, b):
    return lax.dot_general(a, b, (((1,), (1,)), ((), ())), preferred_element_type=F32)


def row_transform(table, value):
    high, low = split(value)
    return dot(table, jnp.concatenate([high, high, low, low], axis=0))


def column_transform(both, table):
    result = dot(both, jnp.concatenate([table, table], axis=0))
    return result[:, :PAIR] + result[:, PAIR:]


def counting(rows, lanes):
    count = lax.broadcasted_iota(jnp.int32, (rows, lanes), 0).astype(F32)
    return count.astype(BF16).reshape(-1, 16, lanes)


def spread(row):
    return jnp.broadcast_to(row, (16, row.shape[1])).astype(BF16)[None]


def flat(tiles):
    return tiles.reshape(-1, tiles.shape[-1])


def frequencies(places):
    return (places // 64).astype(F32), (places % 64).astype(F32)


def lane_part(shape):
    return lax.broadcasted_iota(jnp.int32, shape, 1) // 32


def regroup(members, part):
    result = []
    for start in range(0, GROUP, 4):
        joined = members[start + -part % 4]
        for place in range(1, 4):
            member = members[start + (place - part) % 4]
            joined = jnp.where(lane_part(joined.shape) == place, member, joined)
        result.append(joined)
    return jnp.concatenate(result, axis=1)


def partner(me, count, step):
    return step + (step - me + count) // count


def loop(count, body):
    if count <= 16:
        for step in range(count):
            body(step)
    else:
        lax.fori_loop(0, count, lambda step, carry: (body(step), carry)[1], 0)


def each(count, body):
    if count == 1:
        body(0)
    else:
        lax.fori_loop(0, count, lambda step, carry: (body(step), carry)[1], 0)


def kernel(
    replicas, parts, chunks,
    gradient_ref, momentum_ref, weights_ref, places_hbm, gather_hbm, tables_hbm,
    summed, update, wts, squares,
    grad, mom, places_ref, gather_ref, tables_ref, flipped, row_side, column_high, column_low, both, coefs,
    place_lists, value_lists, low_parts, cell_parts, value_parts, hots, sums,
    in_sem, chunk_sem, place_sem, value_sem, square_sem,
):
    me, mine = lax.axis_index("dp"), lax.axis_index("mp")
    width = summed.shape[1]
    quads = width // QUAD
    per = quads // chunks
    tall = place_lists.shape[1] // chunks

    def block(index):
        return pl.ds(index * QUAD, QUAD)

    def rows(index):
        return pl.ds(index * 64, 64)

    def line(index):
        return index // per * tall + index % per

    def chunk_loads(chunk):
        span = pl.ds(chunk * per * QUAD, per * QUAD)
        return [
            pltpu.make_async_copy(source.at[0, :, span], target.at[:, span], chunk_sem.at[chunk, index])
            for index, (source, target) in enumerate(((gradient_ref, grad), (momentum_ref, mom)))
        ]

    loads = [
        pltpu.make_async_copy(source, target, in_sem.at[index])
        for index, (source, target) in enumerate(
            (
                (places_hbm.at[0, 0], places_ref), (gather_hbm, gather_ref),
                (tables_hbm, tables_ref), (weights_ref, wts),
            )
        )
    ]
    for load in loads[:2]:
        load.start()
    for chunk in range(chunks):
        for load in chunk_loads(chunk):
            load.start()

    barrier = pltpu.get_barrier_semaphore()
    replica = functools.partial(partner, me, replicas)
    other_part = functools.partial(partner, mine, parts)

    def greet_replica(step):
        pl.semaphore_signal(
            barrier, inc=1, device_id={"dp": replica(step)},
            device_id_type=pl.DeviceIdType.MESH,
        )

    def greet_part(step):
        pl.semaphore_signal(
            barrier, inc=1, device_id={"mp": other_part(step)},
            device_id_type=pl.DeviceIdType.MESH,
        )

    loop(replicas - 1, lambda step: greet_replica(replicas - 2 - step))
    loop(parts - 1, greet_part)

    def list_copy(lists, sems, step, slot, span):
        return pltpu.make_async_remote_copy(
            src_ref=lists.at[slot, span], dst_ref=lists.at[slot, span],
            send_sem=sems.at[0], recv_sem=sems.at[1],
            device_id={"dp": replica(step)}, device_id_type=pl.DeviceIdType.MESH,
        )

    def place_copy(step, slot):
        return list_copy(place_lists, place_sem, step, slot, pl.ds(0, (chunks - 1) * tall + per))

    def value_copy(chunk, step, slot):
        return list_copy(value_lists, value_sem.at[chunk], step, slot, pl.ds(chunk * tall, per))

    others = pl.ds(0, replicas - 1)

    groups = place_lists.shape[0] // GROUP
    for slot in range(replicas, groups * GROUP):
        place_lists[slot, :, :] = jnp.zeros(place_lists.shape[1:], F32)
        value_lists[slot, :, :] = jnp.zeros(value_lists.shape[1:], F32)

    loads[0].wait()
    flipped[...] = jnp.transpose(places_ref[...])
    turn = lax.rem(me, 4)
    places = jnp.concatenate(
        [flipped[pl.ds(lax.rem(place + 4 - turn, 4), quads, stride=4), :] for place in range(4)], axis=1
    )
    for chunk in range(chunks):
        place_lists[me, chunk * tall : chunk * tall + per, :] = places[
            chunk * per : (chunk + 1) * per
        ].astype(F32)

    pl.semaphore_wait(barrier, replicas - 1 + parts - 1)
    early = min(replicas - 1, EARLY)
    loop(early, lambda step: place_copy(step, me).start())

    zero, one = jnp.zeros((), BF16), jnp.ones((), BF16)
    count = counting(64, PAIR)
    row_freqs, column_freqs = frequencies(places)
    lanes = lax.rem(lane_part((64, QUAD)) + 4 - turn, 4)

    def hot(row):
        return flat(jnp.where(count == spread(row), one, zero))

    def total(index):
        return 0.9 * mom[:, block(index)] + grad[:, block(index)].astype(F32)

    def column_side(index):
        side = jnp.concatenate([column_high[rows(index), :], column_low[rows(index), :]], axis=1)
        return jnp.concatenate([jnp.where(lanes == part, side, zero) for part in range(4)], axis=0)

    loads[1].wait()
    for index in range(quads):
        pair = [hot(freqs[index : index + 1, :]) for freqs in (row_freqs, column_freqs)]
        both_hot = jnp.concatenate(pair, axis=1)
        found = dot(gather_ref[...], jnp.concatenate([both_hot, both_hot], axis=0))
        row_side[rows(index), :] = found[:, :PAIR]
        column_high[rows(index), :], column_low[rows(index), :] = split(found[:, PAIR:])

    for chunk in range(chunks):
        for load in chunk_loads(chunk):
            load.wait()
        for index in range(chunk * per, (chunk + 1) * per):
            found = dot(jnp.concatenate(split(total(index)), axis=0), column_side(index))
            found = found[:64, :] + found[64:, :]
            found = (found[:, :PAIR] + found[:, PAIR:]) * row_side[rows(index), :]
            value_lists[me, pl.ds(line(index), 1), :] = jnp.sum(found, axis=0, keepdims=True)
        loop(early, lambda step: value_copy(chunk, step, me).start())
        if chunk == 0:
            loop(replicas - 1 - early, lambda step: place_copy(step + early, me).start())
        loop(replicas - 1 - early, lambda step: value_copy(chunk, step + early, me).start())
    for load in loads[2:]:
        load.start()

    def quad(ref, index):
        return jnp.concatenate([ref[rows(2 * index), :], ref[rows(2 * index + 1), :]], axis=1)

    def keep_pair(index, value):
        for half, part in enumerate(split(value)):
            both[rows(index), half * PAIR : (half + 1) * PAIR] = part

    def regroup_places(group):
        low, cell = [], []
        for member in range(GROUP):
            spots = place_lists[group * GROUP + member, :, :].astype(jnp.int32)
            low.append((spots // 64 % 32).astype(F32))
            cell.append((spots // 2048 * 64 + spots % 64).astype(F32))
        for part in range(4):
            low_parts[group, part, :, :] = regroup(low, part)
            cell_parts[group, part, :, :] = regroup(cell, part)

    def regroup_values(group, chunk):
        span = slice(chunk * tall, (chunk + 1) * tall)
        members = [value_lists[group * GROUP + member, span, :] for member in range(GROUP)]
        for part in range(4):
            value_parts[group, part, span, :] = regroup(members, part)

    place_copy(0, others).wait_recv()
    spans = 4 * quads
    count_cell, count_low = counting(PAIR, GROUP * 32), counting(32, GROUP * 32)

    def cells(group, span):
        return pl.ds(pl.multiple_of((group * spans + span) * PAIR, PAIR), PAIR)

    def mark(group):
        regroup_places(group)
        for span in range(spans):
            cell = cell_parts[group, span % 4, pl.ds(line(span // 4), 1), :]
            hots[cells(group, span), :] = flat(
                jnp.where(count_cell == spread(cell), one, zero)
            ).astype(F8)

    def decode(group, span):
        place = pl.ds(line(span // 4), 1)
        here = count_low == spread(low_parts[group, span % 4, place, :])
        halves = split(jnp.broadcast_to(value_parts[group, span % 4, place, :], (16, GROUP * 32)))
        left = jnp.concatenate([flat(jnp.where(here, half[None], zero)) for half in halves], axis=0)
        result = dot_t(left, hots[cells(group, span), :])
        return result[:32, :] + result[32:, :]

    each(groups, mark)

    square = jnp.zeros((8, PAIR), F32)
    for chunk in range(chunks):
        value_copy(chunk, 0, others).wait_recv()
        each(groups, lambda group: regroup_values(group, chunk))
        for span in range(chunk * per * 4, (chunk + 1) * per * 4):
            cells_sum = decode(0, span)
            if groups > 1:
                cells_sum = lax.fori_loop(1, groups, lambda step, acc: acc + decode(step, span), cells_sum)
            square = square + jnp.sum((cells_sum * cells_sum).reshape(4, 8, PAIR), axis=0)
            sums[pl.ds(span * 32, 32), :] = cells_sum

    squares[mine, 0:1, :] = jnp.sum(square, axis=0, keepdims=True)

    def square_copy(step, slot):
        return pltpu.make_async_remote_copy(
            src_ref=squares.at[slot, pl.ds(0, 1)], dst_ref=squares.at[slot, pl.ds(0, 1)],
            send_sem=square_sem.at[0], recv_sem=square_sem.at[1],
            device_id={"mp": other_part(step)}, device_id_type=pl.DeviceIdType.MESH,
        )

    loop(parts - 1, lambda step: square_copy(step, mine).start())

    loads[2].wait()
    first = lane_part((32, PAIR)) < 2
    for pair in range(2 * quads):
        left, right = (sums[pl.ds((2 * pair + side) * 32, 32), :] for side in range(2))
        top = jnp.where(first, left, pltpu.roll(right, 64, axis=1))
        bottom = jnp.where(first, pltpu.roll(left, 64, axis=1), right)
        keep_pair(pair, jnp.concatenate([top, bottom], axis=0))
    coefs[...] = column_transform(both[...], tables_ref[64:, :])
    for index in range(quads):
        update[:, block(index)] = row_transform(tables_ref[:64, :], quad(coefs, index))
    for index in range(quads):
        scaled = row_side[rows(index), :] * value_lists[me, pl.ds(line(index), 1), :]
        high, low = split(scaled)
        left = jnp.concatenate(
            [jnp.concatenate([high, high], axis=1), jnp.concatenate([low, low], axis=1)], axis=0
        )
        back = dot_t(left, column_side(index))
        summed[:, block(index)] = total(index) - (back[:64, :] + back[64:, :])

    loads[3].wait()
    place_copy(0, others).wait_send()
    for chunk in range(chunks):
        value_copy(chunk, 0, others).wait_send()
    square_copy(0, pl.ds(0, parts - 1)).wait()


def deliver(chunks, entries, summed, update, weights, squares, out_momentum_ref, out_weights_ref, result, out_sem):
    share = weights.shape[1] // chunks
    first = pltpu.make_async_copy(summed, out_momentum_ref.at[0], out_sem.at[chunks])
    first.start()
    meansq = jnp.sum(squares[:, 0, :]) / entries
    factor = lax.rsqrt(jnp.full((1, share), meansq + 1.0, F32))
    stores = []
    for chunk in range(chunks):
        span = pl.ds(chunk * share, share)
        result[:, span] = weights[:, span] - update[:, span] * factor
        stores.append(pltpu.make_async_copy(result.at[:, span], out_weights_ref.at[:, span], out_sem.at[chunk]))
        stores[-1].start()
    first.wait()
    for store in stores:
        store.wait()


def local(replicas, parts, gradient, momentum, weights, positions):
    height, width = weights.shape
    quads = width // QUAD
    tables = side_tables()
    anywhere = pl.BlockSpec(memory_space=pl.ANY)
    vmem = pl.BlockSpec(memory_space=pltpu.VMEM)
    chunks = CHUNKS if quads % CHUNKS == 0 else 1
    listed = chunks * (-(-(quads // chunks) // 8) * 8)
    groups = -(-replicas // GROUP)
    entries = positions.shape[-1]
    wide = jax.ShapeDtypeStruct(weights.shape, F32)
    results = pl.pallas_call(
        functools.partial(kernel, replicas, parts, chunks),
        out_shape=(wide, wide, wide, jax.ShapeDtypeStruct((parts, 8, PAIR), F32)),
        in_specs=[pl.BlockSpec(memory_space=pltpu.HBM)] * 6,
        out_specs=(vmem,) * 4,
        scratch_shapes=[
            pltpu.VMEM((height, width), BF16),
            pltpu.VMEM((height, width), F32),
            pltpu.VMEM((entries, 4 * quads), jnp.int32),
            *[pltpu.VMEM(table.shape, BF16) for table in tables],
            pltpu.VMEM((4 * quads, entries), jnp.int32),
            pltpu.VMEM((quads * 64, PAIR), F32),
            pltpu.VMEM((quads * 64, PAIR), BF16),
            pltpu.VMEM((quads * 64, PAIR), BF16),
            pltpu.VMEM((2 * quads * 64, QUAD), BF16),
            pltpu.VMEM((2 * quads * 64, PAIR), F32),
            pltpu.VMEM((groups * GROUP, listed, PAIR), F32),
            pltpu.VMEM((groups * GROUP, listed, PAIR), F32),
            pltpu.VMEM((groups, 4, listed, GROUP * 32), F32),
            pltpu.VMEM((groups, 4, listed, GROUP * 32), F32),
            pltpu.VMEM((groups, 4, listed, GROUP * 32), F32),
            pltpu.VMEM((groups * 4 * quads * PAIR, GROUP * 32), F8),
            pltpu.VMEM((4 * quads * 32, PAIR), F32),
            pltpu.SemaphoreType.DMA((4,)),
            pltpu.SemaphoreType.DMA((chunks, 2)),
            pltpu.SemaphoreType.DMA((2,)),
            pltpu.SemaphoreType.DMA((chunks, 2)),
            pltpu.SemaphoreType.DMA((2,)),
        ],
        compiler_params=pltpu.CompilerParams(
            collective_id=0, has_side_effects=True, vmem_limit_bytes=(22 + 2 * groups) * 1024 * 1024
        ),
    )(
        *(
            pltpu.with_memory_space_constraint(array, pltpu.HBM)
            for array in (
                gradient, momentum, weights, jnp.swapaxes(positions, 2, 3), *map(jnp.asarray, tables),
            )
        )
    )
    return pl.pallas_call(
        functools.partial(deliver, chunks, float(height * width * parts)),
        out_shape=(
            jax.ShapeDtypeStruct(momentum.shape, F32),
            jax.ShapeDtypeStruct(weights.shape, F32),
        ),
        in_specs=[vmem] * 4,
        out_specs=(anywhere, anywhere),
        scratch_shapes=[pltpu.VMEM((height, width), F32), pltpu.SemaphoreType.DMA((chunks + 1,))],
        compiler_params=pltpu.CompilerParams(vmem_limit_bytes=8 * 1024 * 1024),
    )(*results)


def solution(mesh):
    placed = (P("dp", None, "mp"), P("dp", None, "mp"), P(None, "mp"), P("dp", None, "mp", None))
    return jax.shard_map(
        functools.partial(local, mesh.shape["dp"], mesh.shape["mp"]),
        mesh=mesh,
        in_specs=placed,
        out_specs=(P("dp", None, "mp"), P(None, "mp")),
        check_vma=False,
    )
```

```python
import functools

import jax
import jax.numpy as jnp
import numpy as np
from jax import lax
from jax.experimental import pallas as pl
from jax.experimental.pallas import tpu as pltpu
from jax.sharding import PartitionSpec as P

QUAD = 256
PAIR = 128
GROUP = 8
CHUNKS = 1
EARLY = 1
F32 = jnp.float32
BF16 = jnp.bfloat16
F8 = jnp.float8_e4m3fn


def dct_table():
    column = np.arange(64, dtype=np.float64)
    freq = column[:, None]
    factor = np.where(freq == 0, np.sqrt(1.0 / 64), np.sqrt(2.0 / 64))
    return factor * np.cos(np.pi * (2.0 * column[None, :] + 1.0) * freq / 128.0)


def halves(table):
    high = np.asarray(table, np.float32).astype(jnp.bfloat16)
    low = np.asarray(table - high.astype(np.float64), np.float32).astype(jnp.bfloat16)
    return high, low


def side_tables():
    table = dct_table()
    high, low = halves(table.T)
    gather = np.concatenate([high, low], axis=1)
    rows = np.concatenate([high, low, high, low], axis=1)
    columns = np.concatenate(halves(np.kron(np.eye(2), table)), axis=1)
    return gather, np.concatenate([rows, columns], axis=0)


def split(value):
    high = value.astype(BF16)
    return high, (value - high.astype(F32)).astype(BF16)


def dot(a, b):
    return jnp.dot(a, b, preferred_element_type=F32)


def dot_t(a, b):
    return lax.dot_general(a, b, (((1,), (1,)), ((), ())), preferred_element_type=F32)


def row_transform(table, value):
    high, low = split(value)
    return dot(table, jnp.concatenate([high, high, low, low], axis=0))


def column_transform(both, table):
    result = dot(both, jnp.concatenate([table, table], axis=0))
    return result[:, :PAIR] + result[:, PAIR:]


def counting(rows, lanes):
    count = lax.broadcasted_iota(jnp.int32, (rows, lanes), 0).astype(F32)
    return count.astype(BF16).reshape(-1, 16, lanes)


def spread(row):
    return jnp.broadcast_to(row, (16, row.shape[1])).astype(BF16)[None]


def flat(tiles):
    return tiles.reshape(-1, tiles.shape[-1])


def frequencies(places):
    return (places // 64).astype(F32), (places % 64).astype(F32)


def lane_part(shape):
    return lax.broadcasted_iota(jnp.int32, shape, 1) // 32


def regroup(members, part):
    result = []
    for start in range(0, GROUP, 4):
        joined = members[start + -part % 4]
        for place in range(1, 4):
            member = members[start + (place - part) % 4]
            joined = jnp.where(lane_part(joined.shape) == place, member, joined)
        result.append(joined)
    return jnp.concatenate(result, axis=1)


def partner(me, count, step):
    return step + (step - me + count) // count


def loop(count, body):
    if count <= 16:
        for step in range(count):
            body(step)
    else:
        lax.fori_loop(0, count, lambda step, carry: (body(step), carry)[1], 0)


def each(count, body):
    if count == 1:
        body(0)
    else:
        lax.fori_loop(0, count, lambda step, carry: (body(step), carry)[1], 0)


def kernel(
    replicas, parts, chunks,
    gradient_ref, momentum_ref, weights_ref, places_hbm, gather_hbm, tables_hbm,
    summed, update, wts, squares,
    grad, mom, places_ref, gather_ref, tables_ref, flipped, row_side, column_high, column_low, both, coefs,
    place_lists, value_lists, low_parts, cell_parts, value_parts, hots, sums,
    in_sem, chunk_sem, place_sem, value_sem, square_sem,
):
    me, mine = lax.axis_index("dp"), lax.axis_index("mp")
    width = summed.shape[1]
    quads = width // QUAD
    per = quads // chunks
    tall = place_lists.shape[1] // chunks

    def block(index):
        return pl.ds(index * QUAD, QUAD)

    def rows(index):
        return pl.ds(index * 64, 64)

    def line(index):
        return index // per * tall + index % per

    def chunk_loads(chunk):
        span = pl.ds(chunk * per * QUAD, per * QUAD)
        return [
            pltpu.make_async_copy(source.at[0, :, span], target.at[:, span], chunk_sem.at[chunk, index])
            for index, (source, target) in enumerate(((gradient_ref, grad), (momentum_ref, mom)))
        ]

    loads = [
        pltpu.make_async_copy(source, target, in_sem.at[index])
        for index, (source, target) in enumerate(
            (
                (places_hbm.at[0, 0], places_ref), (gather_hbm, gather_ref),
                (tables_hbm, tables_ref), (weights_ref, wts),
            )
        )
    ]
    for load in loads[:2]:
        load.start()

    barrier = pltpu.get_barrier_semaphore()
    replica = functools.partial(partner, me, replicas)
    other_part = functools.partial(partner, mine, parts)

    def greet_replica(step):
        pl.semaphore_signal(
            barrier, inc=1, device_id={"dp": replica(step)},
            device_id_type=pl.DeviceIdType.MESH,
        )

    def greet_part(step):
        pl.semaphore_signal(
            barrier, inc=1, device_id={"mp": other_part(step)},
            device_id_type=pl.DeviceIdType.MESH,
        )

    loop(replicas - 1, lambda step: greet_replica(replicas - 2 - step))
    loop(parts - 1, greet_part)
    for chunk in range(chunks):
        for load in chunk_loads(chunk):
            load.start()

    def list_copy(lists, sems, step, slot, span):
        return pltpu.make_async_remote_copy(
            src_ref=lists.at[slot, span], dst_ref=lists.at[slot, span],
            send_sem=sems.at[0], recv_sem=sems.at[1],
            device_id={"dp": replica(step)}, device_id_type=pl.DeviceIdType.MESH,
        )

    def place_copy(step, slot):
        return list_copy(place_lists, place_sem, step, slot, pl.ds(0, (chunks - 1) * tall + per))

    def value_copy(chunk, step, slot):
        return list_copy(value_lists, value_sem.at[chunk], step, slot, pl.ds(chunk * tall, per))

    others = pl.ds(0, replicas - 1)

    groups = place_lists.shape[0] // GROUP
    for slot in range(replicas, groups * GROUP):
        place_lists[slot, :, :] = jnp.zeros(place_lists.shape[1:], F32)
        value_lists[slot, :, :] = jnp.zeros(value_lists.shape[1:], F32)

    loads[0].wait()
    flipped[...] = jnp.transpose(places_ref[...])
    turn = lax.rem(me, 4)
    places = jnp.concatenate(
        [flipped[pl.ds(lax.rem(place + 4 - turn, 4), quads, stride=4), :] for place in range(4)], axis=1
    )
    for chunk in range(chunks):
        place_lists[me, chunk * tall : chunk * tall + per, :] = places[
            chunk * per : (chunk + 1) * per
        ].astype(F32)

    pl.semaphore_wait(barrier, replicas - 1 + parts - 1)
    early = min(replicas - 1, EARLY)
    loop(early, lambda step: place_copy(step, me).start())

    zero, one = jnp.zeros((), BF16), jnp.ones((), BF16)
    count = counting(64, PAIR)
    row_freqs, column_freqs = frequencies(places)
    lanes = lax.rem(lane_part((64, QUAD)) + 4 - turn, 4)

    def hot(row):
        return flat(jnp.where(count == spread(row), one, zero))

    def total(index):
        return 0.9 * mom[:, block(index)] + grad[:, block(index)].astype(F32)

    def column_side(index):
        side = jnp.concatenate([column_high[rows(index), :], column_low[rows(index), :]], axis=1)
        return jnp.concatenate([jnp.where(lanes == part, side, zero) for part in range(4)], axis=0)

    loads[1].wait()
    for index in range(quads):
        pair = [hot(freqs[index : index + 1, :]) for freqs in (row_freqs, column_freqs)]
        both_hot = jnp.concatenate(pair, axis=1)
        found = dot(gather_ref[...], jnp.concatenate([both_hot, both_hot], axis=0))
        row_side[rows(index), :] = found[:, :PAIR]
        column_high[rows(index), :], column_low[rows(index), :] = split(found[:, PAIR:])

    for chunk in range(chunks):
        for load in chunk_loads(chunk):
            load.wait()
        for index in range(chunk * per, (chunk + 1) * per):
            found = dot(jnp.concatenate(split(total(index)), axis=0), column_side(index))
            found = found[:64, :] + found[64:, :]
            found = (found[:, :PAIR] + found[:, PAIR:]) * row_side[rows(index), :]
            value_lists[me, pl.ds(line(index), 1), :] = jnp.sum(found, axis=0, keepdims=True)
        loop(early, lambda step: value_copy(chunk, step, me).start())
        if chunk == 0:
            loop(replicas - 1 - early, lambda step: place_copy(step + early, me).start())
        loop(replicas - 1 - early, lambda step: value_copy(chunk, step + early, me).start())
    for load in loads[2:]:
        load.start()

    def quad(ref, index):
        return jnp.concatenate([ref[rows(2 * index), :], ref[rows(2 * index + 1), :]], axis=1)

    def keep_pair(index, value):
        for half, part in enumerate(split(value)):
            both[rows(index), half * PAIR : (half + 1) * PAIR] = part

    def regroup_places(group):
        low, cell = [], []
        for member in range(GROUP):
            spots = place_lists[group * GROUP + member, :, :].astype(jnp.int32)
            low.append((spots // 64 % 32).astype(F32))
            cell.append((spots // 2048 * 64 + spots % 64).astype(F32))
        for part in range(4):
            low_parts[group, part, :, :] = regroup(low, part)
            cell_parts[group, part, :, :] = regroup(cell, part)

    def regroup_values(group, chunk):
        span = slice(chunk * tall, (chunk + 1) * tall)
        members = [value_lists[group * GROUP + member, span, :] for member in range(GROUP)]
        for part in range(4):
            value_parts[group, part, span, :] = regroup(members, part)

    place_copy(0, others).wait_recv()
    spans = 4 * quads
    count_cell, count_low = counting(PAIR, GROUP * 32), counting(32, GROUP * 32)

    def cells(group, span):
        return pl.ds(pl.multiple_of((group * spans + span) * PAIR, PAIR), PAIR)

    def mark(group):
        regroup_places(group)
        for span in range(spans):
            cell = cell_parts[group, span % 4, pl.ds(line(span // 4), 1), :]
            hots[cells(group, span), :] = flat(
                jnp.where(count_cell == spread(cell), one, zero)
            ).astype(F8)

    def decode(group, span):
        place = pl.ds(line(span // 4), 1)
        here = count_low == spread(low_parts[group, span % 4, place, :])
        halves = split(jnp.broadcast_to(value_parts[group, span % 4, place, :], (16, GROUP * 32)))
        left = jnp.concatenate([flat(jnp.where(here, half[None], zero)) for half in halves], axis=0)
        result = dot_t(left, hots[cells(group, span), :])
        return result[:32, :] + result[32:, :]

    each(groups, mark)

    square = jnp.zeros((8, PAIR), F32)
    for chunk in range(chunks):
        value_copy(chunk, 0, others).wait_recv()
        each(groups, lambda group: regroup_values(group, chunk))
        for span in range(chunk * per * 4, (chunk + 1) * per * 4):
            cells_sum = decode(0, span)
            if groups > 1:
                cells_sum = lax.fori_loop(1, groups, lambda step, acc: acc + decode(step, span), cells_sum)
            square = square + jnp.sum((cells_sum * cells_sum).reshape(4, 8, PAIR), axis=0)
            sums[pl.ds(span * 32, 32), :] = cells_sum

    squares[mine, 0:1, :] = jnp.sum(square, axis=0, keepdims=True)

    def square_copy(step, slot):
        return pltpu.make_async_remote_copy(
            src_ref=squares.at[slot, pl.ds(0, 1)], dst_ref=squares.at[slot, pl.ds(0, 1)],
            send_sem=square_sem.at[0], recv_sem=square_sem.at[1],
            device_id={"mp": other_part(step)}, device_id_type=pl.DeviceIdType.MESH,
        )

    loop(parts - 1, lambda step: square_copy(step, mine).start())

    loads[2].wait()
    first = lane_part((32, PAIR)) < 2
    for pair in range(2 * quads):
        left, right = (sums[pl.ds((2 * pair + side) * 32, 32), :] for side in range(2))
        top = jnp.where(first, left, pltpu.roll(right, 64, axis=1))
        bottom = jnp.where(first, pltpu.roll(left, 64, axis=1), right)
        keep_pair(pair, jnp.concatenate([top, bottom], axis=0))
    coefs[...] = column_transform(both[...], tables_ref[64:, :])
    for index in range(quads):
        update[:, block(index)] = row_transform(tables_ref[:64, :], quad(coefs, index))
    for index in range(quads):
        scaled = row_side[rows(index), :] * value_lists[me, pl.ds(line(index), 1), :]
        high, low = split(scaled)
        left = jnp.concatenate(
            [jnp.concatenate([high, high], axis=1), jnp.concatenate([low, low], axis=1)], axis=0
        )
        back = dot_t(left, column_side(index))
        summed[:, block(index)] = total(index) - (back[:64, :] + back[64:, :])

    loads[3].wait()
    place_copy(0, others).wait_send()
    for chunk in range(chunks):
        value_copy(chunk, 0, others).wait_send()
    square_copy(0, pl.ds(0, parts - 1)).wait()


def deliver(chunks, entries, summed, update, weights, squares, out_momentum_ref, out_weights_ref, result, out_sem):
    share = weights.shape[1] // chunks
    first = pltpu.make_async_copy(summed, out_momentum_ref.at[0], out_sem.at[chunks])
    first.start()
    meansq = jnp.sum(squares[:, 0, :]) / entries
    factor = lax.rsqrt(jnp.full((1, share), meansq + 1.0, F32))
    stores = []
    for chunk in range(chunks):
        span = pl.ds(chunk * share, share)
        result[:, span] = weights[:, span] - update[:, span] * factor
        stores.append(pltpu.make_async_copy(result.at[:, span], out_weights_ref.at[:, span], out_sem.at[chunk]))
        stores[-1].start()
    first.wait()
    for store in stores:
        store.wait()


def local(replicas, parts, gradient, momentum, weights, positions):
    height, width = weights.shape
    quads = width // QUAD
    tables = side_tables()
    anywhere = pl.BlockSpec(memory_space=pl.ANY)
    vmem = pl.BlockSpec(memory_space=pltpu.VMEM)
    chunks = CHUNKS if quads % CHUNKS == 0 else 1
    listed = chunks * (-(-(quads // chunks) // 8) * 8)
    groups = -(-replicas // GROUP)
    entries = positions.shape[-1]
    wide = jax.ShapeDtypeStruct(weights.shape, F32)
    results = pl.pallas_call(
        functools.partial(kernel, replicas, parts, chunks),
        out_shape=(wide, wide, wide, jax.ShapeDtypeStruct((parts, 8, PAIR), F32)),
        in_specs=[pl.BlockSpec(memory_space=pltpu.HBM)] * 6,
        out_specs=(vmem,) * 4,
        scratch_shapes=[
            pltpu.VMEM((height, width), BF16),
            pltpu.VMEM((height, width), F32),
            pltpu.VMEM((entries, 4 * quads), jnp.int32),
            *[pltpu.VMEM(table.shape, BF16) for table in tables],
            pltpu.VMEM((4 * quads, entries), jnp.int32),
            pltpu.VMEM((quads * 64, PAIR), F32),
            pltpu.VMEM((quads * 64, PAIR), BF16),
            pltpu.VMEM((quads * 64, PAIR), BF16),
            pltpu.VMEM((2 * quads * 64, QUAD), BF16),
            pltpu.VMEM((2 * quads * 64, PAIR), F32),
            pltpu.VMEM((groups * GROUP, listed, PAIR), F32),
            pltpu.VMEM((groups * GROUP, listed, PAIR), F32),
            pltpu.VMEM((groups, 4, listed, GROUP * 32), F32),
            pltpu.VMEM((groups, 4, listed, GROUP * 32), F32),
            pltpu.VMEM((groups, 4, listed, GROUP * 32), F32),
            pltpu.VMEM((groups * 4 * quads * PAIR, GROUP * 32), F8),
            pltpu.VMEM((4 * quads * 32, PAIR), F32),
            pltpu.SemaphoreType.DMA((4,)),
            pltpu.SemaphoreType.DMA((chunks, 2)),
            pltpu.SemaphoreType.DMA((2,)),
            pltpu.SemaphoreType.DMA((chunks, 2)),
            pltpu.SemaphoreType.DMA((2,)),
        ],
        compiler_params=pltpu.CompilerParams(
            collective_id=0, has_side_effects=True, vmem_limit_bytes=(22 + 2 * groups) * 1024 * 1024
        ),
    )(
        *(
            pltpu.with_memory_space_constraint(array, pltpu.HBM)
            for array in (
                gradient, momentum, weights, jnp.swapaxes(positions, 2, 3), *map(jnp.asarray, tables),
            )
        )
    )
    return pl.pallas_call(
        functools.partial(deliver, chunks, float(height * width * parts)),
        out_shape=(
            jax.ShapeDtypeStruct(momentum.shape, F32),
            jax.ShapeDtypeStruct(weights.shape, F32),
        ),
        in_specs=[vmem] * 4,
        out_specs=(anywhere, anywhere),
        scratch_shapes=[pltpu.VMEM((height, width), F32), pltpu.SemaphoreType.DMA((chunks + 1,))],
        compiler_params=pltpu.CompilerParams(vmem_limit_bytes=8 * 1024 * 1024),
    )(*results)


def solution(mesh):
    placed = (P("dp", None, "mp"), P("dp", None, "mp"), P(None, "mp"), P("dp", None, "mp", None))
    return jax.shard_map(
        functools.partial(local, mesh.shape["dp"], mesh.shape["mp"]),
        mesh=mesh,
        in_specs=placed,
        out_specs=(P("dp", None, "mp"), P(None, "mp")),
        check_vma=False,
    )
```
